32 devices in a mesh: gx: 8 (over z, y), gy: 4 (over x, core).
Axes of the slice: x: 2, y: 2, z: 4, core: 2. Of those that a mesh axis runs over, the one named last changes fastest.
Arguments:
- vectors: float32 [64, 32768], P(None, ('gx', 'gy')), may hold values from -6 to 6
- tiles: bfloat16 [4096, 256, 256], P(('gx', 'gy')), may hold values from -0.09375 to 0.09375
- counts: int32 [128], P(('gx', 'gy')), may hold values from 1 to 32, 2112 in all
- tile_col: int32 [4096], P(('gx', 'gy')), may hold values from 0 to 31
- send_list: int32 [32, 32, 1], replicated, may hold values from 0 to 3
Outputs:
- basis: float32 [64, 32768], P(None, ('gx', 'gy'))
- rayleigh: float32 [2, 64, 64], replicated
The draws below stay inside these ranges and needn't reach their ends.
Inputs may be any that keep to these rules, and one draw needn't show every extreme that they name: The first counts[b] of row block b's 32 slots hold its tiles, the others are ignored.
All inputs are finite; a program needn't handle non-finite values.
Results may differ from the reference program's by a relative error of at most 0.0046.
Values may be sent and summed in bfloat16 or wider, within the bound.
No kernel may reach another device: no remote copies, remote signals or barrier semaphores. Data moves between devices by JAX's collectives and lax.ppermute only.
A program may use at most 64 MiB of HBM per device.

```python
import math
import jax
import jax.numpy as jnp
import numpy as np
from jax import lax

K = 64
TILE = 256
RB_DEV = 4
MOST = 32
SEND = 1
ITERS = 2
NB = 128
NROWS = 32768
SLOTS = 4096
DEVICES = 32


def set_ends(drawn, key, low, largest):
    index_at = [jax.random.randint(jax.random.fold_in(key, axis), (), 0, length) for axis, length in enumerate(drawn.shape)]
    widest = drawn.shape.index(max(drawn.shape))
    beside = index_at[:widest] + [(index_at[widest] + 1) % drawn.shape[widest]] + index_at[widest + 1:]
    return drawn.at[tuple(index_at)].set(low).at[tuple(beside)].set(largest)


def block_levels(stream_key, dims, pieces, smallest, largest):
    def one(dim, shards_of):
        steps = jax.random.uniform(jax.random.fold_in(jax.random.fold_in(stream_key, 6), dim), (shards_of,), jnp.float32, smallest / len(pieces), largest / len(pieces))
        return jnp.repeat(jnp.exp(steps), dims[dim] // shards_of).reshape((-1,) + (1,) * (len(dims) - dim - 1))

    loudness = one(*pieces[0])
    for cut in pieces[1:]:
        loudness = loudness * one(*cut)
    return loudness


def profile(count, total, most, lean):
    portions = [(1 << 20) // math.isqrt(grade ** lean) + 1 for grade in range(2, count + 1)]
    surplus, given = total - most - (count - 1), [1] * (count - 1)
    while surplus > 0:
        movable = [i for i in range(count - 1) if given[i] < most]
        whole, budget = sum([portions[i] for i in movable]), surplus
        for i in movable:
            more = min(most - given[i], max(1, budget * portions[i] // whole), surplus)
            given[i] = given[i] + more
            surplus = surplus - more
    return np.array([most] + given)


def uneven(key, count, total, most, skew):
    if count == 2:
        one = jax.random.randint(key, (), max(1, total - most), min(most, total - 1) + 1)
        return jnp.stack([one, total - one])
    sizes = jnp.asarray(profile(count, total, most, skew), jnp.int32)
    twos = (count - 1) // 2
    donor, taker = sizes[1:1 + 2 * twos:2], sizes[2:2 + 2 * twos:2]
    room = jnp.minimum(donor - 1, most - taker)
    moved = jax.random.randint(jax.random.fold_in(key, 1), (twos,), 0, 1 << 20) % (room + 1)
    sizes = sizes.at[1:1 + 2 * twos:2].set(donor - moved).at[2:2 + 2 * twos:2].set(taker + moved)
    return sizes[jax.random.permutation(jax.random.fold_in(key, 2), count)]


def gaussian(key, dims, width, bound, cuts=(), kind=jnp.bfloat16):
    array = width * jax.random.normal(key, dims, jnp.float32)
    if cuts:
        array = array * block_levels(key, dims, cuts, -0.22, 0.18)
    return jnp.clip(array, -bound, bound).astype(kind)


def setup_inputs(seed: int = 0) -> dict:
    splits = jax.random.split(jax.random.key(seed), 6)
    return {
        "vectors": gaussian(splits[0], (K, NROWS), 1.0, 6.0, ((1, 32),), jnp.float32),
        "tiles": gaussian(splits[1], (SLOTS, TILE, TILE), (TILE * (MOST + 1) // 2) ** -0.5, 0.09375, ((0, 32),)),
        "counts": uneven(splits[2], NB, NB * (MOST + 1) // 2, MOST, 2).astype(jnp.int32),
        "tile_col": set_ends(jax.random.randint(splits[3], (SLOTS,), 0, DEVICES * SEND), jax.random.fold_in(splits[3], 1), 0, (DEVICES * SEND) - 1).astype(jnp.int32),
        "send_list": set_ends(jax.random.randint(splits[4], (DEVICES, DEVICES, SEND), 0, RB_DEV), jax.random.fold_in(splits[4], 1), 0, RB_DEV - 1).astype(jnp.int32),
    }


def reference(vectors, tiles, counts, tile_col, send_list):
    ndev = NB // RB_DEV
    tiles_dev = tiles.reshape(ndev, RB_DEV * MOST, TILE, TILE)
    cols = tile_col.reshape(ndev, RB_DEV * MOST)
    cnt = counts.reshape(ndev, RB_DEV)
    live = ((jnp.arange(RB_DEV * MOST, dtype=jnp.int32) % MOST)[None, :] < jnp.repeat(cnt, MOST, axis=1)).astype(jnp.float32)
    source = (cols // SEND).astype(jnp.int32)
    sslot = (cols % SEND).astype(jnp.int32)
    receiver = jnp.arange(ndev, dtype=jnp.int32)[:, None]
    gcol = (source * RB_DEV + send_list[source, receiver, sslot]).astype(jnp.int32)
    current = vectors
    rayleigh = []
    for step in range(ITERS):
        rounded = current.astype(jnp.bfloat16)
        blocks = rounded.reshape(K, NB, TILE)

        def one_device(items):
            tile_set, columns, mask = items
            picked = blocks[:, columns, :].astype(jnp.float32)
            prod = jnp.einsum('jrc,kjc->jkr', tile_set.astype(jnp.float32), picked, precision=lax.Precision.HIGHEST)
            prod = prod * mask[:, None, None]
            return prod.reshape(RB_DEV, MOST, K, TILE).sum(axis=1)
        out = lax.map(one_device, (tiles_dev, gcol, live))
        image = out.transpose(2, 0, 1, 3).reshape(K, NROWS)
        gram = jnp.dot(image, image.T, precision=lax.Precision.HIGHEST) / NROWS
        rayleigh.append(jnp.dot(current, image.T, precision=lax.Precision.HIGHEST) / jnp.sqrt(jnp.float32(NROWS)))
        lower = jnp.linalg.cholesky(gram)
        current = lax.linalg.triangular_solve(lower, image, left_side=True, lower=True)
    return (current, jnp.stack(rayleigh))
```

```python
import functools

import jax
import jax.numpy as jnp
from jax import lax
from jax.experimental import pallas as pl
from jax.experimental.pallas import tpu as pltpu
from jax.sharding import PartitionSpec as P

ITERS = 2
AXES = ("gx", "gy")
F32 = jnp.float32
BF16 = jnp.bfloat16
HIGHEST = lax.Precision.HIGHEST

GAIN_LIMIT = 1.5
SMALL, LARGE = 1e-25, 1e25


def vmem():
    return pl.BlockSpec(memory_space=pltpu.VMEM)


def smem():
    return pl.BlockSpec(memory_space=pltpu.SMEM)


def nt_dot(a, b, precision=None):
    return lax.dot_general(
        a, b, (((1,), (1,)), ((), ())), precision=precision, preferred_element_type=F32
    )


def pack_kernel(outgoing, vectors, parcel, rounded):
    tile = parcel.shape[2]
    for b in range(vectors.shape[1] // tile):
        rounded[b] = vectors[:, b * tile : (b + 1) * tile].astype(BF16)

    def one(p, carry):
        parcel[p] = rounded[outgoing[p]]
        return carry

    lax.fori_loop(0, parcel.shape[0], one, 0)


def pack(outgoing, vectors, tile):
    width, rows = vectors.shape
    return pl.pallas_call(
        pack_kernel,
        out_shape=jax.ShapeDtypeStruct((outgoing.shape[0], width, tile), BF16),
        in_specs=[smem(), vmem()],
        out_specs=vmem(),
        scratch_shapes=[pltpu.VMEM((rows // tile, width, tile), BF16)],
        compiler_params=pltpu.CompilerParams(vmem_limit_bytes=24 << 20),
    )(outgoing, vectors)


def image_kernel(send, counts, cols, outgoing, arrived, before, tiles, *rest):
    if send:
        image, parcel, sums, held, total, rounded, sems = rest
    else:
        image, sums, held, total, sems = rest
    blocks = counts.shape[0]
    depth = tiles.shape[0] // blocks
    tile = tiles.shape[1]

    def fetch(slot):
        return pltpu.make_async_copy(tiles.at[slot], held.at[slot], sems.at[slot])

    def fetch_block(b):
        def one(t, carry):
            fetch(b * depth + t).start()
            return carry

        lax.fori_loop(0, counts[b], one, 0)

    def product(slot):
        return nt_dot(held[slot], arrived[cols[slot]])

    fetch_block(0)
    if blocks > 1:
        fetch_block(1)
    for b in range(blocks):
        if b + 2 < blocks:
            fetch_block(b + 2)
        total[...] = jnp.zeros_like(total)
        fours = counts[b] // 4

        def four(g, carry):
            slot = b * depth + 4 * g
            for i in range(4):
                fetch(slot + i).wait()
            total[...] += (product(slot) + product(slot + 1)) + (
                product(slot + 2) + product(slot + 3)
            )
            return carry

        def single(t, carry):
            slot = b * depth + t
            fetch(slot).wait()
            total[...] += product(slot)
            return carry

        lax.fori_loop(0, fours, four, 0)
        lax.fori_loop(4 * fours, counts[b], single, 0)
        block = total[...].T
        image[:, b * tile : (b + 1) * tile] = block
        if send:
            rounded[b] = block.astype(BF16)
    if send:

        def one(p, carry):
            parcel[p] = rounded[outgoing[p]]
            return carry

        lax.fori_loop(0, parcel.shape[0], one, 0)
    both = jnp.concatenate([image[...], before[...]], axis=0)
    sums[...] = nt_dot(image[...], both, HIGHEST)


def image_of(send, counts, cols, outgoing, arrived, before, tiles):
    devices, width, tile = arrived.shape
    rows = before.shape[1]
    image = jax.ShapeDtypeStruct((width, rows), F32)
    sums = jax.ShapeDtypeStruct((width, 2 * width), F32)
    parcel = jax.ShapeDtypeStruct((devices, width, tile), BF16)
    scratch = [pltpu.VMEM(tiles.shape, BF16), pltpu.VMEM((tile, width), F32)]
    if send:
        scratch.append(pltpu.VMEM((rows // tile, width, tile), BF16))
    scratch.append(pltpu.SemaphoreType.DMA((tiles.shape[0],)))
    return pl.pallas_call(
        functools.partial(image_kernel, send),
        out_shape=(image, parcel, sums) if send else (image, sums),
        in_specs=[smem(), smem(), smem(), vmem(), vmem(), pl.BlockSpec(memory_space=pl.ANY)],
        out_specs=(vmem(),) * (3 if send else 2),
        scratch_shapes=scratch,
        compiler_params=pltpu.CompilerParams(vmem_limit_bytes=40 << 20),
        cost_estimate=pl.CostEstimate(
            flops=width * tile * tile * tiles.shape[0],
            bytes_accessed=tiles.shape[0] * tile * tile,
            transcendentals=0,
        ),
    )(counts, cols, outgoing, arrived, before, tiles)


def inverse_factor(a):
    n = a.shape[0]
    row = lax.broadcasted_iota(jnp.int32, (n, 2 * n), 0)
    lane = lax.broadcasted_iota(jnp.int32, (n, 2 * n), 1)
    eye = (lane == row + n).astype(F32)
    m = jnp.concatenate([a, eye[:, n:]], axis=1)
    for j in range(n - 1):
        factor = m[:, j : j + 1] / m[j : j + 1, j : j + 1]
        m = m - jnp.where(row > j, factor, 0.0) * m[j : j + 1, :]
    pivots = jnp.sum(jnp.where(lane == row, m, 0.0), axis=1, keepdims=True)
    return m[:, n:] / jnp.sqrt(pivots)


def diagonal(a):
    n = a.shape[0]
    row = lax.broadcasted_iota(jnp.int32, (n, n), 0)
    lane = lax.broadcasted_iota(jnp.int32, (n, n), 1)
    return jnp.sum(jnp.where(row == lane, a, 0.0), axis=0, keepdims=True)


def in_range(d):
    return (jnp.min(d) > SMALL) & (jnp.max(d) < LARGE)


def first_kernel(total_rows, sums, inverse, gain):
    n = sums.shape[0]
    gram = sums[:, :n] * (1.0 / total_rows)
    x = inverse_factor(gram)
    inverse[...] = x
    d = diagonal(gram)
    value = jnp.sum(x * x * d) * (1.0 / n)
    gain[0] = jnp.where(in_range(d), value, jnp.inf)


def last_kernel(total_rows, sums1, inverse1, gain, sums2, inverse2, rayleigh, good):
    n = sums1.shape[0]
    gram = sums2[:, :n] * (1.0 / total_rows)
    x = inverse_factor(gram)
    inverse2[...] = x
    scale = 1.0 / (total_rows**0.5)
    rayleigh[0] = sums1[:, n:].T * scale
    right = nt_dot(sums2[:, n:].T, inverse1[...], HIGHEST)
    rayleigh[1] = jnp.dot(inverse1[...], right, precision=HIGHEST) * scale
    d = diagonal(gram)
    fine = in_range(d) & (jnp.max(jnp.abs(x)) < LARGE) & (gain[0] < GAIN_LIMIT)
    good[0] = fine.astype(jnp.int32)


def sum_everywhere(value, devices):
    if devices & (devices - 1):
        return lax.psum(value, AXES)

    def from_peer(v, mask):
        return lax.ppermute(v, AXES, [(i, i ^ mask) for i in range(devices)])

    bits = devices.bit_length() - 1
    bit = 0
    if bits % 2:
        value = value + from_peer(value, 1)
        bit = 1
    while bit < bits:
        a, b = 1 << bit, 2 << bit
        value = (value + from_peer(value, a)) + (from_peer(value, b) + from_peer(value, a | b))
        bit += 2
    return value


def step_by_step(vectors, tiles, counts, tile_col, outgoing):
    devices = lax.axis_size(AXES)
    width, rows_here = vectors.shape
    blocks_here = counts.shape[0]
    tile_size = tiles.shape[1]
    depth = tiles.shape[0] // blocks_here
    total_rows = rows_here * devices
    live = jnp.arange(tiles.shape[0], dtype=jnp.int32) % depth < jnp.repeat(counts, depth)
    live = live.astype(F32)
    current = vectors
    rayleigh = []
    for step in range(ITERS):
        rounded = current.astype(BF16)
        own_blocks = rounded.reshape(width, blocks_here, tile_size).transpose(1, 0, 2)
        parcel = jnp.take(own_blocks, outgoing, axis=0)
        arrived = lax.all_to_all(parcel, AXES, split_axis=0, concat_axis=0, tiled=True)
        picked = jnp.take(arrived, tile_col, axis=0)
        prod = jnp.einsum("jrc,jkc->jkr", tiles, picked, preferred_element_type=F32)
        prod = prod * live[:, None, None]
        image = prod.reshape(blocks_here, depth, width, tile_size).sum(axis=1)
        image = image.transpose(1, 0, 2).reshape(width, rows_here)
        gram_part = jnp.dot(image, image.T, precision=HIGHEST)
        quotient_part = jnp.dot(current, image.T, precision=HIGHEST)
        gram, quotient = lax.psum((gram_part, quotient_part), AXES)
        gram = gram / total_rows
        rayleigh.append(quotient / jnp.sqrt(F32(total_rows)))
        lower = jnp.linalg.cholesky(gram)
        current = lax.linalg.triangular_solve(lower, image, left_side=True, lower=True)
    return current, jnp.stack(rayleigh)


def on_device(vectors, tiles, counts, tile_col, send_list):
    me = lax.axis_index(AXES)
    devices = lax.axis_size(AXES)
    width, rows_here = vectors.shape
    total_rows = rows_here * devices
    outgoing = lax.dynamic_index_in_dim(send_list, me, 0, keepdims=False).reshape(-1)

    def exchange(parcel):
        return lax.all_to_all(parcel, AXES, split_axis=0, concat_axis=0, tiled=True)

    square = jax.ShapeDtypeStruct((width, width), F32)
    arrived = exchange(pack(outgoing, vectors, tiles.shape[1]))
    image1, parcel, sums1 = image_of(True, counts, tile_col, outgoing, arrived, vectors, tiles)
    arrived = exchange(parcel)
    sums1 = sum_everywhere(sums1, devices)
    inverse1, gain = pl.pallas_call(
        functools.partial(first_kernel, total_rows),
        out_shape=(square, jax.ShapeDtypeStruct((1,), F32)),
        in_specs=[vmem()],
        out_specs=(vmem(), smem()),
    )(sums1)
    image2, sums2 = image_of(False, counts, tile_col, outgoing, arrived, image1, tiles)
    sums2 = sum_everywhere(sums2, devices)
    inverse2, rayleigh, good = pl.pallas_call(
        functools.partial(last_kernel, total_rows),
        out_shape=(
            square,
            jax.ShapeDtypeStruct((2, width, width), F32),
            jax.ShapeDtypeStruct((1,), jnp.int32),
        ),
        in_specs=[vmem(), vmem(), smem(), vmem()],
        out_specs=(vmem(), vmem(), smem()),
    )(sums1, inverse1, gain, sums2)

    def fast():
        return jnp.dot(inverse2, image2, precision=HIGHEST), rayleigh

    def slow():
        return step_by_step(vectors, tiles, counts, tile_col, outgoing)

    return lax.cond(good[0] > 0, fast, slow)


def solution(mesh):
    return jax.shard_map(
        on_device,
        mesh=mesh,
        in_specs=(
            P(None, AXES),
            P(AXES, None, None),
            P(AXES),
            P(AXES),
            P(),
        ),
        out_specs=(P(None, AXES), P()),
        check_vma=False,
    )
```

```python
import functools

import jax
import jax.numpy as jnp
from jax import lax
from jax.experimental import pallas as pl
from jax.experimental.pallas import tpu as pltpu
from jax.sharding import PartitionSpec as P

ITERS = 2
AXES = ("gx", "gy")
F32 = jnp.float32
BF16 = jnp.bfloat16
HIGHEST = lax.Precision.HIGHEST

GAIN_LIMIT = 1.5
SMALL, LARGE = 1e-25, 1e25
STEP = 4


def vmem():
    return pl.BlockSpec(memory_space=pltpu.VMEM)


def smem():
    return pl.BlockSpec(memory_space=pltpu.SMEM)


def nt_dot(a, b, precision=None):
    return lax.dot_general(
        a, b, (((1,), (1,)), ((), ())), precision=precision, preferred_element_type=F32
    )


def pack_kernel(outgoing, vectors, parcel, rounded):
    tile = parcel.shape[2]
    for b in range(vectors.shape[1] // tile):
        rounded[b] = vectors[:, b * tile : (b + 1) * tile].astype(BF16)

    def one(p, carry):
        parcel[p] = rounded[outgoing[p]]
        return carry

    lax.fori_loop(0, parcel.shape[0], one, 0)


def pack(outgoing, vectors, tile):
    width, rows = vectors.shape
    return pl.pallas_call(
        pack_kernel,
        out_shape=jax.ShapeDtypeStruct((outgoing.shape[0], width, tile), BF16),
        in_specs=[smem(), vmem()],
        out_specs=vmem(),
        scratch_shapes=[pltpu.VMEM((rows // tile, width, tile), BF16)],
        compiler_params=pltpu.CompilerParams(vmem_limit_bytes=24 << 20),
    )(outgoing, vectors)


def image_kernel(send, counts, cols, outgoing, arrived, tiles, image, *rest):
    if send:
        parcel, held, turned, rounded, sems = rest
    else:
        held, turned, sems = rest
    blocks = counts.shape[0]
    depth = tiles.shape[0] // blocks
    tile = tiles.shape[1]
    width = image.shape[0]
    mxus = (0, 1)

    def steps_of(b):
        return (counts[b] + STEP - 1) // STEP

    def fetch(b, q):
        slots = pl.ds(b * depth + q * STEP, STEP)
        return pltpu.make_async_copy(tiles.at[slots], held.at[slots], sems.at[b * (depth // STEP) + q])

    for b in range(blocks):

        def start(q, carry):
            fetch(b, q).start()
            return carry

        lax.fori_loop(0, steps_of(b), start, 0)

    def stage(b, t, register, mxu):
        slot = jnp.minimum(b * depth + t, blocks * depth - 1)
        block = arrived[cols[slot]]
        block = jnp.where(t < counts[b], block, jnp.zeros_like(block))
        block = jnp.concatenate([block, jnp.zeros((tile - width, tile), BF16)], axis=0)
        pltpu.matmul_push_rhs(block, staging_register=register, mxu_index=mxu, transpose=True)

    def multiply(*refs):
        sums = (refs[0:2], refs[2:4])
        spare = refs[4:6]
        for ref in refs:
            pltpu.matmul_pop(ref)
        for mxu in mxus:
            stage(0, mxu, 0, mxu)

        def flush(b):
            first, second = sums[b % 2]
            turned[b] = (pltpu.matmul_pop(first) + pltpu.matmul_pop(second))[:, :width]

        for b in range(blocks):
            steps = steps_of(b)

            def step(q, carry):
                fetch(b, q).wait()
                t = q * STEP
                slot = b * depth + t
                last = q == steps - 1
                for mxu in mxus:
                    stage(b, t + 2 + mxu, 1, mxu)
                for mxu in mxus:
                    pltpu.matmul_acc_lhs(sums[b % 2][mxu], held[slot + mxu], load_staged_rhs=0)
                for mxu in mxus:
                    if b + 1 < blocks:
                        stage(jnp.where(last, b + 1, b), jnp.where(last, mxu, t + STEP + mxu), 0, mxu)
                    else:
                        stage(b, t + STEP + mxu, 0, mxu)
                for mxu in mxus:
                    pltpu.matmul_acc_lhs(sums[b % 2][mxu], held[slot + 2 + mxu], load_staged_rhs=1)
                return carry

            lax.fori_loop(0, steps, step, 0)
            if b:
                flush(b - 1)
        for mxu in mxus:
            pltpu.matmul_acc_lhs(spare[mxu], jnp.zeros((16, tile), BF16), load_staged_rhs=0)
        flush(blocks - 1)
        for ref in spare:
            pltpu.matmul_pop(ref)

    pl.run_scoped(
        multiply,
        *[pltpu.ACC(mxu)((tile, tile), F32) for mxu in mxus + mxus],
        *[pltpu.ACC(mxu)((16, tile), F32) for mxu in mxus],
    )
    for b in range(blocks):
        block = turned[b].T
        image[:, b * tile : (b + 1) * tile] = block
        if send:
            rounded[b] = block.astype(BF16)
    if send:

        def one(p, carry):
            parcel[p] = rounded[outgoing[p]]
            return carry

        lax.fori_loop(0, parcel.shape[0], one, 0)


def image_of(send, counts, cols, outgoing, arrived, tiles):
    senders, width, tile = arrived.shape
    blocks = counts.shape[0]
    assert tiles.shape[0] % (blocks * STEP) == 0 and tile == 256 and width <= 128
    image = jax.ShapeDtypeStruct((width, blocks * tile), F32)
    parcel = jax.ShapeDtypeStruct((senders, width, tile), BF16)
    scratch = [pltpu.VMEM(tiles.shape, BF16), pltpu.VMEM((blocks, tile, width), F32)]
    if send:
        scratch.append(pltpu.VMEM((blocks, width, tile), BF16))
    scratch.append(pltpu.SemaphoreType.DMA((tiles.shape[0] // STEP,)))
    return pl.pallas_call(
        functools.partial(image_kernel, send),
        out_shape=(image, parcel) if send else image,
        in_specs=[smem(), smem(), smem(), vmem(), pl.BlockSpec(memory_space=pl.ANY)],
        out_specs=(vmem(), vmem()) if send else vmem(),
        scratch_shapes=scratch,
        compiler_params=pltpu.CompilerParams(vmem_limit_bytes=40 << 20),
        cost_estimate=pl.CostEstimate(
            flops=width * tiles.size, bytes_accessed=tiles.size, transcendentals=0
        ),
    )(counts, cols, outgoing, arrived, tiles)


def sums_of(image, before):
    both = jnp.concatenate([image, before], axis=0)
    return nt_dot(image, both, HIGHEST)


def inverse_factor(a):
    n = a.shape[0]
    row = lax.broadcasted_iota(jnp.int32, (n, 2 * n), 0)
    lane = lax.broadcasted_iota(jnp.int32, (n, 2 * n), 1)
    eye = (lane == row + n).astype(F32)
    m = jnp.concatenate([a, eye[:, n:]], axis=1)
    for j in range(n - 1):
        factor = m[:, j : j + 1] / m[j : j + 1, j : j + 1]
        m = m - jnp.where(row > j, factor, 0.0) * m[j : j + 1, :]
    pivots = jnp.sum(jnp.where(lane == row, m, 0.0), axis=1, keepdims=True)
    return m[:, n:] / jnp.sqrt(pivots)


def diagonal(a):
    n = a.shape[0]
    row = lax.broadcasted_iota(jnp.int32, (n, n), 0)
    lane = lax.broadcasted_iota(jnp.int32, (n, n), 1)
    return jnp.sum(jnp.where(row == lane, a, 0.0), axis=0, keepdims=True)


def in_range(d):
    return (jnp.min(d) > SMALL) & (jnp.max(d) < LARGE)


def first_kernel(total_rows, sums, inverse, gain):
    n = sums.shape[0]
    gram = sums[:, :n] * (1.0 / total_rows)
    x = inverse_factor(gram)
    inverse[...] = x
    d = diagonal(gram)
    value = jnp.sum(x * x * d) * (1.0 / n)
    gain[0] = jnp.where(in_range(d), value, jnp.inf)


def last_kernel(total_rows, sums1, inverse1, gain, sums2, inverse2, rayleigh, good):
    n = sums1.shape[0]
    gram = sums2[:, :n] * (1.0 / total_rows)
    x = inverse_factor(gram)
    inverse2[...] = x
    scale = 1.0 / (total_rows**0.5)
    rayleigh[0] = sums1[:, n:].T * scale
    right = nt_dot(sums2[:, n:].T, inverse1[...], HIGHEST)
    rayleigh[1] = jnp.dot(inverse1[...], right, precision=HIGHEST) * scale
    d = diagonal(gram)
    fine = in_range(d) & (jnp.max(jnp.abs(x)) < LARGE) & (gain[0] < GAIN_LIMIT)
    good[0] = fine.astype(jnp.int32)


def sum_everywhere(value, devices):
    if devices & (devices - 1):
        return lax.psum(value, AXES)

    def from_peer(v, mask):
        return lax.ppermute(v, AXES, [(i, i ^ mask) for i in range(devices)])

    bits = devices.bit_length() - 1
    bit = 0
    if bits % 2:
        value = value + from_peer(value, 1)
        bit = 1
    while bit < bits:
        a, b = 1 << bit, 2 << bit
        value = (value + from_peer(value, a)) + (from_peer(value, b) + from_peer(value, a | b))
        bit += 2
    return value


def step_by_step(vectors, tiles, counts, tile_col, outgoing):
    devices = lax.axis_size(AXES)
    width, rows_here = vectors.shape
    blocks_here = counts.shape[0]
    tile_size = tiles.shape[1]
    depth = tiles.shape[0] // blocks_here
    total_rows = rows_here * devices
    live = jnp.arange(tiles.shape[0], dtype=jnp.int32) % depth < jnp.repeat(counts, depth)
    live = live.astype(F32)
    current = vectors
    rayleigh = []
    for step in range(ITERS):
        rounded = current.astype(BF16)
        own_blocks = rounded.reshape(width, blocks_here, tile_size).transpose(1, 0, 2)
        parcel = jnp.take(own_blocks, outgoing, axis=0)
        arrived = lax.all_to_all(parcel, AXES, split_axis=0, concat_axis=0, tiled=True)
        picked = jnp.take(arrived, tile_col, axis=0)
        prod = jnp.einsum("jrc,jkc->jkr", tiles, picked, preferred_element_type=F32)
        prod = prod * live[:, None, None]
        image = prod.reshape(blocks_here, depth, width, tile_size).sum(axis=1)
        image = image.transpose(1, 0, 2).reshape(width, rows_here)
        gram_part = jnp.dot(image, image.T, precision=HIGHEST)
        quotient_part = jnp.dot(current, image.T, precision=HIGHEST)
        gram, quotient = lax.psum((gram_part, quotient_part), AXES)
        gram = gram / total_rows
        rayleigh.append(quotient / jnp.sqrt(F32(total_rows)))
        lower = jnp.linalg.cholesky(gram)
        current = lax.linalg.triangular_solve(lower, image, left_side=True, lower=True)
    return current, jnp.stack(rayleigh)


def on_device(vectors, tiles, counts, tile_col, send_list):
    me = lax.axis_index(AXES)
    devices = lax.axis_size(AXES)
    width, rows_here = vectors.shape
    total_rows = rows_here * devices
    outgoing = lax.dynamic_index_in_dim(send_list, me, 0, keepdims=False).reshape(-1)

    def exchange(parcel):
        return lax.all_to_all(parcel, AXES, split_axis=0, concat_axis=0, tiled=True)

    square = jax.ShapeDtypeStruct((width, width), F32)
    arrived = exchange(pack(outgoing, vectors, tiles.shape[1]))
    image1, parcel = image_of(True, counts, tile_col, outgoing, arrived, tiles)
    arrived = exchange(parcel)
    sums1 = sum_everywhere(sums_of(image1, vectors), devices)
    inverse1, gain = pl.pallas_call(
        functools.partial(first_kernel, total_rows),
        out_shape=(square, jax.ShapeDtypeStruct((1,), F32)),
        in_specs=[vmem()],
        out_specs=(vmem(), smem()),
    )(sums1)
    arrived, inverse1 = lax.optimization_barrier((arrived, inverse1))
    image2 = image_of(False, counts, tile_col, outgoing, arrived, tiles)
    sums2 = sums_of(image2, image1)
    sums2 = sum_everywhere(sums2, devices)
    inverse2, rayleigh, good = pl.pallas_call(
        functools.partial(last_kernel, total_rows),
        out_shape=(
            square,
            jax.ShapeDtypeStruct((2, width, width), F32),
            jax.ShapeDtypeStruct((1,), jnp.int32),
        ),
        in_specs=[vmem(), vmem(), smem(), vmem()],
        out_specs=(vmem(), vmem(), smem()),
    )(sums1, inverse1, gain, sums2)

    def fast():
        return jnp.dot(inverse2, image2, precision=HIGHEST), rayleigh

    def slow():
        return step_by_step(vectors, tiles, counts, tile_col, outgoing)

    return lax.cond(good[0] > 0, fast, slow)


def solution(mesh):
    return jax.shard_map(
        on_device,
        mesh=mesh,
        in_specs=(
            P(None, AXES),
            P(AXES, None, None),
            P(AXES),
            P(AXES),
            P(),
        ),
        out_specs=(P(None, AXES), P()),
        check_vma=False,
    )
```

```python
import functools

import jax
import jax.numpy as jnp
from jax import lax
from jax.experimental import pallas as pl
from jax.experimental.pallas import tpu as pltpu
from jax.sharding import PartitionSpec as P

ITERS = 2
AXES = ("gx", "gy")
F32 = jnp.float32
BF16 = jnp.bfloat16
HIGHEST = lax.Precision.HIGHEST

GAIN_LIMIT = 1.5
SMALL, LARGE = 1e-25, 1e25
STEP = 4


def vmem():
    return pl.BlockSpec(memory_space=pltpu.VMEM)


def smem():
    return pl.BlockSpec(memory_space=pltpu.SMEM)


def nt_dot(a, b, precision=None):
    return lax.dot_general(
        a, b, (((1,), (1,)), ((), ())), precision=precision, preferred_element_type=F32
    )


def pack_kernel(outgoing, vectors, parcel, rounded):
    tile = parcel.shape[2]
    for b in range(vectors.shape[1] // tile):
        rounded[b] = vectors[:, b * tile : (b + 1) * tile].astype(BF16)

    def one(p, carry):
        parcel[p] = rounded[outgoing[p]]
        return carry

    lax.fori_loop(0, parcel.shape[0], one, 0)


def pack(outgoing, vectors, tile):
    width, rows = vectors.shape
    return pl.pallas_call(
        pack_kernel,
        out_shape=jax.ShapeDtypeStruct((outgoing.shape[0], width, tile), BF16),
        in_specs=[smem(), vmem()],
        out_specs=vmem(),
        scratch_shapes=[pltpu.VMEM((rows // tile, width, tile), BF16)],
        compiler_params=pltpu.CompilerParams(vmem_limit_bytes=24 << 20),
    )(outgoing, vectors)


def image_kernel(send, counts, cols, outgoing, arrived, tiles, image, *rest):
    if send:
        parcel, held, turned, rounded, sems = rest
    else:
        held, turned, sems = rest
    blocks = counts.shape[0]
    depth = tiles.shape[0] // blocks
    tile = tiles.shape[1]
    width = image.shape[0]
    mxus = (0, 1)

    def steps_of(b):
        return (counts[b] + STEP - 1) // STEP

    def fetch(b, q):
        slots = pl.ds(b * depth + q * STEP, STEP)
        return pltpu.make_async_copy(tiles.at[slots], held.at[slots], sems.at[b * (depth // STEP) + q])

    for b in range(blocks):

        def start(q, carry):
            fetch(b, q).start()
            return carry

        lax.fori_loop(0, steps_of(b), start, 0)

    def stage(b, t, register, mxu):
        slot = jnp.minimum(b * depth + t, blocks * depth - 1)
        block = arrived[cols[slot]]
        block = jnp.where(t < counts[b], block, jnp.zeros_like(block))
        block = jnp.concatenate([block, jnp.zeros((tile - width, tile), BF16)], axis=0)
        pltpu.matmul_push_rhs(block, staging_register=register, mxu_index=mxu, transpose=True)

    def multiply(*refs):
        sums = (refs[0:2], refs[2:4])
        spare = refs[4:6]
        for ref in refs:
            pltpu.matmul_pop(ref)
        for mxu in mxus:
            stage(0, mxu, 0, mxu)

        def flush(b):
            first, second = sums[b % 2]
            turned[b] = (pltpu.matmul_pop(first) + pltpu.matmul_pop(second))[:, :width]

        for b in range(blocks):
            steps = steps_of(b)

            def step(q, carry):
                fetch(b, q).wait()
                t = q * STEP
                slot = b * depth + t
                last = q == steps - 1
                for mxu in mxus:
                    stage(b, t + 2 + mxu, 1, mxu)
                for mxu in mxus:
                    pltpu.matmul_acc_lhs(sums[b % 2][mxu], held[slot + mxu], load_staged_rhs=0)
                for mxu in mxus:
                    if b + 1 < blocks:
                        stage(jnp.where(last, b + 1, b), jnp.where(last, mxu, t + STEP + mxu), 0, mxu)
                    else:
                        stage(b, t + STEP + mxu, 0, mxu)
                for mxu in mxus:
                    pltpu.matmul_acc_lhs(sums[b % 2][mxu], held[slot + 2 + mxu], load_staged_rhs=1)
                return carry

            lax.fori_loop(0, steps, step, 0)
            if b:
                flush(b - 1)
        for mxu in mxus:
            pltpu.matmul_acc_lhs(spare[mxu], jnp.zeros((16, tile), BF16), load_staged_rhs=0)
        flush(blocks - 1)
        for ref in spare:
            pltpu.matmul_pop(ref)

    pl.run_scoped(
        multiply,
        *[pltpu.ACC(mxu)((tile, tile), F32) for mxu in mxus + mxus],
        *[pltpu.ACC(mxu)((16, tile), F32) for mxu in mxus],
    )
    for b in range(blocks):
        block = turned[b].T
        image[:, b * tile : (b + 1) * tile] = block
        if send:
            rounded[b] = block.astype(BF16)
    if send:

        def one(p, carry):
            parcel[p] = rounded[outgoing[p]]
            return carry

        lax.fori_loop(0, parcel.shape[0], one, 0)


def image_of(send, counts, cols, outgoing, arrived, tiles):
    senders, width, tile = arrived.shape
    blocks = counts.shape[0]
    assert tiles.shape[0] % (blocks * STEP) == 0 and tile == 256 and width <= 128
    image = jax.ShapeDtypeStruct((width, blocks * tile), F32)
    parcel = jax.ShapeDtypeStruct((senders, width, tile), BF16)
    scratch = [pltpu.VMEM(tiles.shape, BF16), pltpu.VMEM((blocks, tile, width), F32)]
    if send:
        scratch.append(pltpu.VMEM((blocks, width, tile), BF16))
    scratch.append(pltpu.SemaphoreType.DMA((tiles.shape[0] // STEP,)))
    return pl.pallas_call(
        functools.partial(image_kernel, send),
        out_shape=(image, parcel) if send else image,
        in_specs=[smem(), smem(), smem(), vmem(), pl.BlockSpec(memory_space=pl.ANY)],
        out_specs=(vmem(), vmem()) if send else vmem(),
        scratch_shapes=scratch,
        compiler_params=pltpu.CompilerParams(vmem_limit_bytes=40 << 20),
        cost_estimate=pl.CostEstimate(
            flops=width * tiles.size, bytes_accessed=tiles.size, transcendentals=0
        ),
    )(counts, cols, outgoing, arrived, tiles)


def sums_kernel(vectors, image1, image2, sums):
    n = vectors.shape[0]
    first = jnp.concatenate([image1[...], vectors[...]], axis=0)
    second = jnp.concatenate([image2[...], image1[...]], axis=0)
    sums[:, : 2 * n] = nt_dot(image1[...], first, HIGHEST)
    sums[:, 2 * n :] = nt_dot(image2[...], second, HIGHEST)


def sums_of(vectors, image1, image2):
    n = vectors.shape[0]
    return pl.pallas_call(
        sums_kernel,
        out_shape=jax.ShapeDtypeStruct((n, 4 * n), F32),
        in_specs=[vmem()] * 3,
        out_specs=vmem(),
        compiler_params=pltpu.CompilerParams(vmem_limit_bytes=16 << 20),
    )(vectors, image1, image2)


def inverse_factors(grams):
    n = grams[0].shape[0]
    wide = 2 * n
    group = 8
    pieces = n // group
    sub = lax.broadcasted_iota(jnp.int32, (group, wide), 0)
    lane = lax.broadcasted_iota(jnp.int32, (group, wide), 1)

    def spread(row):
        return jnp.broadcast_to(row, (group, wide))

    held = []
    for a in grams:
        rows = []
        for r in range(pieces):
            eye = (lane == sub + (n + group * r)).astype(F32)[:, n:]
            rows.append(jnp.concatenate([a[group * r : group * (r + 1), :], eye], axis=1))
        held.append(rows)
    pivots = [[] for _ in grams]
    for k in range(pieces):
        columns = [
            [[spread(m[r][:, j : j + 1]) for r in range(k, pieces)] for j in range(group * k, group * (k + 1))]
            for m in held
        ]
        found = [jnp.ones((group, wide), F32) for _ in grams]
        for j in range(group):
            for p, m in enumerate(held):
                column = columns[p]
                pivot = spread(column[j][0][j : j + 1, :])
                found[p] = jnp.where(sub == j, pivot, found[p])
                row = spread(m[k][j : j + 1, :]) / pivot
                later = [spread(column[i][0][j : j + 1, :]) / pivot for i in range(j + 1, group)]
                for r in range(k, pieces):
                    factor = column[j][r - k]
                    if r == k:
                        factor = jnp.where(sub > j, factor, 0.0)
                    m[r] = m[r] - factor * row
                    for i in range(j + 1, group):
                        column[i][r - k] = column[i][r - k] - factor * later[i - j - 1]
        for p in range(len(grams)):
            pivots[p].append(found[p])
    return [
        jnp.concatenate(
            [(held[p][r] / jnp.sqrt(pivots[p][r]))[:, n:] for r in range(pieces)], axis=0
        )
        for p in range(len(grams))
    ]


def diagonal(a):
    n = a.shape[0]
    row = lax.broadcasted_iota(jnp.int32, (n, n), 0)
    lane = lax.broadcasted_iota(jnp.int32, (n, n), 1)
    return jnp.sum(jnp.where(row == lane, a, 0.0), axis=0, keepdims=True)


def in_range(d):
    return (jnp.min(d) > SMALL) & (jnp.max(d) < LARGE)


def factor_kernel(total_rows, sums, inverse2, rayleigh, good):
    n = inverse2.shape[0]
    scale = 1.0 / (total_rows**0.5)
    gram1, gram2 = [sums[:, i * n : (i + 1) * n] * (1.0 / total_rows) for i in (0, 2)]
    x1, x2 = inverse_factors([gram1, gram2])
    inverse2[...] = x2
    rayleigh[0] = sums[:, n : 2 * n].T * scale
    right = nt_dot(sums[:, 3 * n :].T, x1, HIGHEST)
    rayleigh[1] = jnp.dot(x1, right, precision=HIGHEST, preferred_element_type=F32) * scale
    d1 = diagonal(gram1)
    gain = jnp.sum(x1 * x1 * d1) * (1.0 / n)
    fine = in_range(d1) & in_range(diagonal(gram2)) & (gain < GAIN_LIMIT)
    good[0] = (fine & (jnp.max(jnp.abs(x2)) < LARGE)).astype(jnp.int32)


def factor(total_rows, sums):
    n = sums.shape[0]
    return pl.pallas_call(
        functools.partial(factor_kernel, total_rows),
        out_shape=(
            jax.ShapeDtypeStruct((n, n), F32),
            jax.ShapeDtypeStruct((2, n, n), F32),
            jax.ShapeDtypeStruct((1,), jnp.int32),
        ),
        in_specs=[vmem()],
        out_specs=(vmem(), vmem(), smem()),
    )(sums)


def sum_everywhere(value, devices):
    if devices & (devices - 1):
        return lax.psum(value, AXES)

    def from_peer(v, mask):
        return lax.ppermute(v, AXES, [(i, i ^ mask) for i in range(devices)])

    bits = devices.bit_length() - 1
    bit = 0
    if bits % 2:
        value = value + from_peer(value, 1)
        bit = 1
    while bit < bits:
        a, b = 1 << bit, 2 << bit
        value = (value + from_peer(value, a)) + (from_peer(value, b) + from_peer(value, a | b))
        bit += 2
    return value


def step_by_step(vectors, tiles, counts, tile_col, outgoing):
    devices = lax.axis_size(AXES)
    width, rows_here = vectors.shape
    blocks_here = counts.shape[0]
    tile_size = tiles.shape[1]
    depth = tiles.shape[0] // blocks_here
    total_rows = rows_here * devices
    live = jnp.arange(tiles.shape[0], dtype=jnp.int32) % depth < jnp.repeat(counts, depth)
    live = live.astype(F32)
    current = vectors
    rayleigh = []
    for step in range(ITERS):
        rounded = current.astype(BF16)
        own_blocks = rounded.reshape(width, blocks_here, tile_size).transpose(1, 0, 2)
        parcel = jnp.take(own_blocks, outgoing, axis=0)
        arrived = lax.all_to_all(parcel, AXES, split_axis=0, concat_axis=0, tiled=True)
        picked = jnp.take(arrived, tile_col, axis=0)
        prod = jnp.einsum("jrc,jkc->jkr", tiles, picked, preferred_element_type=F32)
        prod = prod * live[:, None, None]
        image = prod.reshape(blocks_here, depth, width, tile_size).sum(axis=1)
        image = image.transpose(1, 0, 2).reshape(width, rows_here)
        gram_part = jnp.dot(image, image.T, precision=HIGHEST)
        quotient_part = jnp.dot(current, image.T, precision=HIGHEST)
        gram, quotient = lax.psum((gram_part, quotient_part), AXES)
        gram = gram / total_rows
        rayleigh.append(quotient / jnp.sqrt(F32(total_rows)))
        lower = jnp.linalg.cholesky(gram)
        current = lax.linalg.triangular_solve(lower, image, left_side=True, lower=True)
    return current, jnp.stack(rayleigh)


def on_device(vectors, tiles, counts, tile_col, send_list):
    me = lax.axis_index(AXES)
    devices = lax.axis_size(AXES)
    width, rows_here = vectors.shape
    total_rows = rows_here * devices
    outgoing = lax.dynamic_index_in_dim(send_list, me, 0, keepdims=False).reshape(-1)

    def exchange(parcel):
        return lax.all_to_all(parcel, AXES, split_axis=0, concat_axis=0, tiled=True)

    arrived = exchange(pack(outgoing, vectors, tiles.shape[1]))
    image1, parcel = image_of(True, counts, tile_col, outgoing, arrived, tiles)
    image2 = image_of(False, counts, tile_col, outgoing, exchange(parcel), tiles)
    sums = sum_everywhere(sums_of(vectors, image1, image2), devices)
    inverse2, rayleigh, good = factor(total_rows, sums)

    def fast():
        return jnp.dot(inverse2, image2, precision=HIGHEST), rayleigh

    def slow():
        return step_by_step(vectors, tiles, counts, tile_col, outgoing)

    return lax.cond(good[0] > 0, fast, slow)


def solution(mesh):
    return jax.shard_map(
        on_device,
        mesh=mesh,
        in_specs=(
            P(None, AXES),
            P(AXES, None, None),
            P(AXES),
            P(AXES),
            P(),
        ),
        out_specs=(P(None, AXES), P()),
        check_vma=False,
    )
```

```python
import functools

import jax
import jax.numpy as jnp
from jax import lax
from jax.experimental import pallas as pl
from jax.experimental.pallas import tpu as pltpu
from jax.sharding import PartitionSpec as P

ITERS = 2
AXES = ("gx", "gy")
F32 = jnp.float32
BF16 = jnp.bfloat16
HIGHEST = lax.Precision.HIGHEST

GAIN_LIMIT = 1.5
SMALL, LARGE = 1e-25, 1e25
STEP = 4


def vmem():
    return pl.BlockSpec(memory_space=pltpu.VMEM)


def smem():
    return pl.BlockSpec(memory_space=pltpu.SMEM)


def nt_dot(a, b, precision=None):
    return lax.dot_general(
        a, b, (((1,), (1,)), ((), ())), precision=precision, preferred_element_type=F32
    )


def pack_kernel(outgoing, own, other, parcel):
    peers, rows, tile = parcel.shape
    width = own.shape[0]
    slots = rows // width // 2

    def one(p, carry):
        for i, source in enumerate((own, other)):
            for slot in range(slots):
                block = outgoing[(i * peers + p) * slots + slot]
                at = (i * slots + slot) * width
                parcel[p, at : at + width, :] = source[:, pl.ds(pl.multiple_of(block * tile, tile), tile)]
        return carry

    lax.fori_loop(0, peers, one, 0)


def pack(outgoing, own, other, peers, tile):
    width = own.shape[0]
    rows = outgoing.shape[0] // peers * width
    return pl.pallas_call(
        pack_kernel,
        out_shape=jax.ShapeDtypeStruct((peers, rows, tile), BF16),
        in_specs=[smem(), vmem(), vmem()],
        out_specs=vmem(),
        compiler_params=pltpu.CompilerParams(vmem_limit_bytes=16 << 20),
    )(outgoing, own, other)


class Exchange:
    def __init__(self, devices, send_list, tile):
        assert devices >= 4 and devices & (devices - 1) == 0
        self.half = devices // 2
        self.mask = 3 * (devices // 4)
        self.swap = [(i, i ^ self.mask) for i in range(devices)]
        self.groups = [list(range(self.half)), list(range(self.half, devices))]
        self.tile = tile
        self.slots = send_list.shape[2]
        me = lax.axis_index(AXES)
        self.base = me // self.half * self.half
        lists = [
            lax.dynamic_slice(send_list, (source, self.base, 0), (1, self.half, self.slots))
            for source in (me, me ^ self.mask)
        ]
        self.outgoing = jnp.concatenate(lists).reshape(-1)

    def arrival(self, tile_col):
        sender, slot = tile_col // self.slots, tile_col % self.slots
        far = (sender < self.base) | (sender >= self.base + self.half)
        near = jnp.where(far, sender ^ self.mask, sender) - self.base
        return (2 * near + far.astype(jnp.int32)) * self.slots + slot

    def __call__(self, rounded, *ahead):
        other = lax.ppermute(rounded, AXES, self.swap)
        parcel = pack(self.outgoing, rounded, other, self.half, self.tile)
        parcel, *_ = lax.optimization_barrier((parcel, *ahead))
        arrived = lax.all_to_all(
            parcel, AXES, split_axis=0, concat_axis=0, axis_index_groups=self.groups, tiled=True
        )
        return arrived.reshape(-1, rounded.shape[0], self.tile)


def steps_of(count):
    return (count + STEP - 1) // STEP


def stage_kernel(counts, tiles, held, sems):
    blocks = counts.shape[0]
    depth = tiles.shape[0] // blocks

    def each(act):
        for b in range(blocks):

            def one(q, carry):
                slots = pl.ds(b * depth + q * STEP, STEP)
                act(pltpu.make_async_copy(tiles.at[slots], held.at[slots], sems.at[b * (depth // STEP) + q]))
                return carry

            lax.fori_loop(0, steps_of(counts[b]), one, 0)

    each(lambda copy: copy.start())
    each(lambda copy: copy.wait())


def stage(counts, tiles):
    return pl.pallas_call(
        stage_kernel,
        out_shape=pltpu.MemorySpace.VMEM(tiles.shape, tiles.dtype),
        in_specs=[smem(), pl.BlockSpec(memory_space=pl.ANY)],
        out_specs=vmem(),
        scratch_shapes=[pltpu.SemaphoreType.DMA((tiles.shape[0] // STEP,))],
        compiler_params=pltpu.CompilerParams(vmem_limit_bytes=4 << 20),
        cost_estimate=pl.CostEstimate(
            flops=5_000_000_000, bytes_accessed=2 * tiles.size, transcendentals=0
        ),
    )(counts, tiles)


def image_kernel(counts, cols, arrived, tiles, image, *rest):
    rounded, turned = rest if len(rest) == 2 else (None, rest[0])
    blocks = counts.shape[0]
    depth = tiles.shape[0] // blocks
    tile = tiles.shape[1]
    width = image.shape[0]
    mxus = (0, 1)

    def stage(b, t, register, mxu):
        slot = jnp.minimum(b * depth + t, blocks * depth - 1)
        block = arrived[cols[slot]]
        block = jnp.where(t < counts[b], block, jnp.zeros_like(block))
        block = jnp.concatenate([block, jnp.zeros((tile - width, tile), BF16)], axis=0)
        pltpu.matmul_push_rhs(block, staging_register=register, mxu_index=mxu, transpose=True)

    def multiply(*refs):
        sums = (refs[0:2], refs[2:4])
        spare = refs[4:6]
        for ref in refs:
            pltpu.matmul_pop(ref)
        for mxu in mxus:
            stage(0, mxu, 0, mxu)

        def flush(b):
            first, second = sums[b % 2]
            turned[b] = (pltpu.matmul_pop(first) + pltpu.matmul_pop(second))[:, :width]

        for b in range(blocks):
            steps = steps_of(counts[b])

            def step(q, carry):
                t = q * STEP
                slot = b * depth + t
                last = q == steps - 1
                for mxu in mxus:
                    stage(b, t + 2 + mxu, 1, mxu)
                for mxu in mxus:
                    pltpu.matmul_acc_lhs(sums[b % 2][mxu], tiles[slot + mxu], load_staged_rhs=0)
                for mxu in mxus:
                    if b + 1 < blocks:
                        stage(jnp.where(last, b + 1, b), jnp.where(last, mxu, t + STEP + mxu), 0, mxu)
                    else:
                        stage(b, t + STEP + mxu, 0, mxu)
                for mxu in mxus:
                    pltpu.matmul_acc_lhs(sums[b % 2][mxu], tiles[slot + 2 + mxu], load_staged_rhs=1)
                return carry

            lax.fori_loop(0, steps, step, 0)
            if b:
                flush(b - 1)
        for mxu in mxus:
            pltpu.matmul_acc_lhs(spare[mxu], jnp.zeros((16, tile), BF16), load_staged_rhs=0)
        flush(blocks - 1)
        for ref in spare:
            pltpu.matmul_pop(ref)

    pl.run_scoped(
        multiply,
        *[pltpu.ACC(mxu)((tile, tile), F32) for mxu in mxus + mxus],
        *[pltpu.ACC(mxu)((16, tile), F32) for mxu in mxus],
    )
    for b in range(blocks):
        block = turned[b].T
        image[:, b * tile : (b + 1) * tile] = block
        if rounded is not None:
            rounded[:, b * tile : (b + 1) * tile] = block.astype(BF16)


def image_of(send, counts, cols, arrived, tiles):
    width, tile = arrived.shape[1:]
    blocks = counts.shape[0]
    assert tiles.shape[0] % (blocks * STEP) == 0 and tile == 256 and width <= 128
    image = jax.ShapeDtypeStruct((width, blocks * tile), F32)
    rounded = jax.ShapeDtypeStruct((width, blocks * tile), BF16)
    return pl.pallas_call(
        image_kernel,
        out_shape=(image, rounded) if send else image,
        in_specs=[smem(), smem(), vmem(), vmem()],
        out_specs=(vmem(), vmem()) if send else vmem(),
        scratch_shapes=[pltpu.VMEM((blocks, tile, width), F32)],
        compiler_params=pltpu.CompilerParams(vmem_limit_bytes=24 << 20),
        cost_estimate=pl.CostEstimate(
            flops=width * tiles.size, bytes_accessed=tiles.size, transcendentals=0
        ),
    )(counts, cols, arrived, tiles)


def sums_kernel(vectors, image1, image2, sums):
    n = vectors.shape[0]
    first = jnp.concatenate([image1[...], vectors[...]], axis=0)
    second = jnp.concatenate([image2[...], image1[...]], axis=0)
    sums[:, : 2 * n] = nt_dot(image1[...], first, HIGHEST)
    sums[:, 2 * n :] = nt_dot(image2[...], second, HIGHEST)


def sums_of(vectors, image1, image2):
    n = vectors.shape[0]
    return pl.pallas_call(
        sums_kernel,
        out_shape=jax.ShapeDtypeStruct((n, 4 * n), F32),
        in_specs=[vmem()] * 3,
        out_specs=vmem(),
        compiler_params=pltpu.CompilerParams(vmem_limit_bytes=16 << 20),
    )(vectors, image1, image2)


def inverse_factors(grams):
    n = grams[0].shape[0]
    wide = 2 * n
    group = 8
    pieces = n // group
    sub = lax.broadcasted_iota(jnp.int32, (group, wide), 0)
    lane = lax.broadcasted_iota(jnp.int32, (group, wide), 1)

    def spread(row):
        return jnp.broadcast_to(row, (group, wide))

    held = []
    for a in grams:
        rows = []
        for r in range(pieces):
            eye = (lane == sub + (n + group * r)).astype(F32)[:, n:]
            rows.append(jnp.concatenate([a[group * r : group * (r + 1), :], eye], axis=1))
        held.append(rows)
    pivots = [[] for _ in grams]
    for k in range(pieces):
        columns = [
            [[spread(m[r][:, j : j + 1]) for r in range(k, pieces)] for j in range(group * k, group * (k + 1))]
            for m in held
        ]
        found = [jnp.ones((group, wide), F32) for _ in grams]
        for j in range(group):
            for p, m in enumerate(held):
                column = columns[p]
                pivot = spread(column[j][0][j : j + 1, :])
                found[p] = jnp.where(sub == j, pivot, found[p])
                row = spread(m[k][j : j + 1, :]) / pivot
                later = [spread(column[i][0][j : j + 1, :]) / pivot for i in range(j + 1, group)]
                for r in range(k, pieces):
                    factor = column[j][r - k]
                    if r == k:
                        factor = jnp.where(sub > j, factor, 0.0)
                    m[r] = m[r] - factor * row
                    for i in range(j + 1, group):
                        column[i][r - k] = column[i][r - k] - factor * later[i - j - 1]
        for p in range(len(grams)):
            pivots[p].append(found[p])
    return [
        jnp.concatenate(
            [(held[p][r] / jnp.sqrt(pivots[p][r]))[:, n:] for r in range(pieces)], axis=0
        )
        for p in range(len(grams))
    ]


def diagonal(a):
    n = a.shape[0]
    row = lax.broadcasted_iota(jnp.int32, (n, n), 0)
    lane = lax.broadcasted_iota(jnp.int32, (n, n), 1)
    return jnp.sum(jnp.where(row == lane, a, 0.0), axis=0, keepdims=True)


def in_range(d):
    return (jnp.min(d) > SMALL) & (jnp.max(d) < LARGE)


def factor_kernel(total_rows, sums, inverse2, rayleigh, good):
    n = inverse2.shape[0]
    scale = 1.0 / (total_rows**0.5)
    gram1, gram2 = [sums[:, i * n : (i + 1) * n] * (1.0 / total_rows) for i in (0, 2)]
    x1, x2 = inverse_factors([gram1, gram2])
    inverse2[...] = x2
    rayleigh[0] = sums[:, n : 2 * n].T * scale
    right = nt_dot(sums[:, 3 * n :].T, x1, HIGHEST)
    rayleigh[1] = jnp.dot(x1, right, precision=HIGHEST, preferred_element_type=F32) * scale
    d1 = diagonal(gram1)
    gain = jnp.sum(x1 * x1 * d1) * (1.0 / n)
    fine = in_range(d1) & in_range(diagonal(gram2)) & (gain < GAIN_LIMIT)
    good[0] = (fine & (jnp.max(jnp.abs(x2)) < LARGE)).astype(jnp.int32)


def factor(total_rows, sums):
    n = sums.shape[0]
    return pl.pallas_call(
        functools.partial(factor_kernel, total_rows),
        out_shape=(
            jax.ShapeDtypeStruct((n, n), F32),
            jax.ShapeDtypeStruct((2, n, n), F32),
            jax.ShapeDtypeStruct((1,), jnp.int32),
        ),
        in_specs=[vmem()],
        out_specs=(vmem(), vmem(), smem()),
    )(sums)


def sum_everywhere(value, devices):
    if devices & (devices - 1):
        return lax.psum(value, AXES)

    def from_peer(v, mask):
        return lax.ppermute(v, AXES, [(i, i ^ mask) for i in range(devices)])

    bits = devices.bit_length() - 1
    bit = 0
    if bits % 2:
        value = value + from_peer(value, 1)
        bit = 1
    while bit < bits:
        a, b = 1 << bit, 2 << bit
        value = (value + from_peer(value, a)) + (from_peer(value, b) + from_peer(value, a | b))
        bit += 2
    return value


def step_by_step(vectors, tiles, counts, tile_col, send_list):
    me = lax.axis_index(AXES)
    outgoing = lax.dynamic_index_in_dim(send_list, me, 0, keepdims=False).reshape(-1)
    devices = lax.axis_size(AXES)
    width, rows_here = vectors.shape
    blocks_here = counts.shape[0]
    tile_size = tiles.shape[1]
    depth = tiles.shape[0] // blocks_here
    total_rows = rows_here * devices
    live = jnp.arange(tiles.shape[0], dtype=jnp.int32) % depth < jnp.repeat(counts, depth)
    live = live.astype(F32)
    current = vectors
    rayleigh = []
    for step in range(ITERS):
        rounded = current.astype(BF16)
        own_blocks = rounded.reshape(width, blocks_here, tile_size).transpose(1, 0, 2)
        parcel = jnp.take(own_blocks, outgoing, axis=0)
        arrived = lax.all_to_all(parcel, AXES, split_axis=0, concat_axis=0, tiled=True)
        picked = jnp.take(arrived, tile_col, axis=0)
        prod = jnp.einsum("jrc,jkc->jkr", tiles, picked, preferred_element_type=F32)
        prod = prod * live[:, None, None]
        image = prod.reshape(blocks_here, depth, width, tile_size).sum(axis=1)
        image = image.transpose(1, 0, 2).reshape(width, rows_here)
        gram_part = jnp.dot(image, image.T, precision=HIGHEST)
        quotient_part = jnp.dot(current, image.T, precision=HIGHEST)
        gram, quotient = lax.psum((gram_part, quotient_part), AXES)
        gram = gram / total_rows
        rayleigh.append(quotient / jnp.sqrt(F32(total_rows)))
        lower = jnp.linalg.cholesky(gram)
        current = lax.linalg.triangular_solve(lower, image, left_side=True, lower=True)
    return current, jnp.stack(rayleigh)


def on_device(vectors, tiles, counts, tile_col, send_list):
    devices = lax.axis_size(AXES)
    total_rows = vectors.shape[1] * devices
    exchange = Exchange(devices, send_list, tiles.shape[1])
    cols = exchange.arrival(tile_col)
    held = stage(counts, tiles)
    arrived = exchange(vectors.astype(BF16), cols, held)
    image1, rounded = image_of(True, counts, cols, arrived, held)
    image2 = image_of(False, counts, cols, exchange(rounded), held)
    sums = sum_everywhere(sums_of(vectors, image1, image2), devices)
    inverse2, rayleigh, good = factor(total_rows, sums)

    def fast():
        return jnp.dot(inverse2, image2, precision=HIGHEST), rayleigh

    def slow():
        return step_by_step(vectors, tiles, counts, tile_col, send_list)

    return lax.cond(good[0] > 0, fast, slow)


def solution(mesh):
    return jax.shard_map(
        on_device,
        mesh=mesh,
        in_specs=(
            P(None, AXES),
            P(AXES, None, None),
            P(AXES),
            P(AXES),
            P(),
        ),
        out_specs=(P(None, AXES), P()),
        check_vma=False,
    )
```

```python
import functools

import jax
import jax.numpy as jnp
from jax import lax
from jax.experimental import pallas as pl
from jax.experimental.pallas import tpu as pltpu
from jax.sharding import PartitionSpec as P

ITERS = 2
AXES = ("gx", "gy")
F32 = jnp.float32
BF16 = jnp.bfloat16
HIGHEST = lax.Precision.HIGHEST

GAIN_LIMIT = 1.5
SMALL, LARGE = 1e-25, 1e25
STEP = 4


def vmem():
    return pl.BlockSpec(memory_space=pltpu.VMEM)


def smem():
    return pl.BlockSpec(memory_space=pltpu.SMEM)


def nt_dot(a, b, precision=None):
    return lax.dot_general(
        a, b, (((1,), (1,)), ((), ())), precision=precision, preferred_element_type=F32
    )


def pack_kernel(outgoing, own, other, parcel):
    peers, rows, tile = parcel.shape
    width = own.shape[0]
    slots = rows // width // 2

    def one(p, carry):
        for i, source in enumerate((own, other)):
            for slot in range(slots):
                block = outgoing[(i * peers + p) * slots + slot]
                at = (i * slots + slot) * width
                parcel[p, at : at + width, :] = source[:, pl.ds(pl.multiple_of(block * tile, tile), tile)]
        return carry

    lax.fori_loop(0, peers, one, 0)


def pack(outgoing, own, other, peers, tile):
    width = own.shape[0]
    rows = outgoing.shape[0] // peers * width
    return pl.pallas_call(
        pack_kernel,
        out_shape=jax.ShapeDtypeStruct((peers, rows, tile), BF16),
        in_specs=[smem(), vmem(), vmem()],
        out_specs=vmem(),
        compiler_params=pltpu.CompilerParams(vmem_limit_bytes=4 << 20),
        cost_estimate=pl.CostEstimate(
            flops=5_000_000_000, bytes_accessed=32 << 20, transcendentals=0
        ),
    )(outgoing, own, other)


class Exchange:
    def __init__(self, devices, send_list, tile):
        assert devices >= 4 and devices & (devices - 1) == 0
        self.half = devices // 2
        self.mask = 3 * (devices // 4)
        self.swap = [(i, i ^ self.mask) for i in range(devices)]
        self.groups = [list(range(self.half)), list(range(self.half, devices))]
        self.tile = tile
        self.slots = send_list.shape[2]
        me = lax.axis_index(AXES)
        self.base = me // self.half * self.half
        lists = [
            lax.dynamic_slice(send_list, (source, self.base, 0), (1, self.half, self.slots))
            for source in (me, me ^ self.mask)
        ]
        self.outgoing = jnp.concatenate(lists).reshape(-1)

    def arrival(self, tile_col):
        sender, slot = tile_col // self.slots, tile_col % self.slots
        far = (sender < self.base) | (sender >= self.base + self.half)
        near = jnp.where(far, sender ^ self.mask, sender) - self.base
        return (2 * near + far.astype(jnp.int32)) * self.slots + slot

    def __call__(self, rounded, *ahead):
        other = lax.ppermute(rounded, AXES, self.swap)
        parcel = pack(self.outgoing, rounded, other, self.half, self.tile)
        parcel, *_ = lax.optimization_barrier((parcel, *ahead))
        arrived = lax.all_to_all(
            parcel, AXES, split_axis=0, concat_axis=0, axis_index_groups=self.groups, tiled=True
        )
        return arrived.reshape(-1, rounded.shape[0], self.tile)


def image_kernel(counts, cols, arrived, tiles, image, *rounded):
    blocks = counts.shape[0]
    depth = tiles.shape[0] // blocks
    tile = tiles.shape[1]
    width = arrived.shape[1]
    mxus = (0, 1)

    def push(b, t, register, mxu):
        pltpu.matmul_push_rhs(
            tiles[b * depth + t], staging_register=register, mxu_index=mxu, transpose=True
        )

    def block(b, t):
        found = arrived[cols[b * depth + t]]
        return jnp.where(t < counts[b], found, jnp.zeros_like(found))

    def run(*refs):
        sums = (refs[0:2], refs[2:4])
        spare = refs[4:6]
        for ref in refs:
            pltpu.matmul_pop(ref)

        def flush(b):
            first, second = sums[b % 2]
            value = pltpu.matmul_pop(first) + pltpu.matmul_pop(second)
            for ref in (image, *rounded):
                ref[:, b * tile : (b + 1) * tile] = value.astype(ref.dtype)

        for mxu in mxus:
            push(0, mxu, 0, mxu)
        for b in range(blocks):
            steps = (counts[b] + STEP - 1) // STEP

            def products(t, push_next):
                for mxu in mxus:
                    push(b, t + 2 + mxu, 1, mxu)
                for mxu in mxus:
                    pltpu.matmul_acc_lhs(sums[b % 2][mxu], block(b, t + mxu), load_staged_rhs=0)
                for mxu in mxus:
                    push_next(mxu)
                for mxu in mxus:
                    pltpu.matmul_acc_lhs(sums[b % 2][mxu], block(b, t + 2 + mxu), load_staged_rhs=1)

            def step(q, carry):
                products(q * STEP, lambda mxu: push(b, (q + 1) * STEP + mxu, 0, mxu))
                return carry

            lax.fori_loop(0, steps - 1, step, 0)
            products((steps - 1) * STEP, lambda mxu: push(min(b + 1, blocks - 1), mxu, 0, mxu))
            if b:
                flush(b - 1)
        for mxu in mxus:
            pltpu.matmul_acc_lhs(spare[mxu], jnp.zeros((16, tile), BF16), load_staged_rhs=0)
        flush(blocks - 1)
        for ref in spare:
            pltpu.matmul_pop(ref)

    pl.run_scoped(
        run,
        *[pltpu.ACC(mxu)((width, tile), F32) for mxu in mxus + mxus],
        *[pltpu.ACC(mxu)((16, tile), F32) for mxu in mxus],
    )


def image_of(kinds, counts, cols, arrived, tiles):
    width, tile = arrived.shape[1:]
    blocks = counts.shape[0]
    assert tile == 256 and width % 16 == 0 and width <= 256
    assert tiles.shape[0] % (blocks * STEP) == 0
    return pl.pallas_call(
        image_kernel,
        out_shape=[jax.ShapeDtypeStruct((width, blocks * tile), kind) for kind in kinds],
        in_specs=[smem(), smem(), vmem(), vmem()],
        out_specs=[vmem()] * len(kinds),
        compiler_params=pltpu.CompilerParams(vmem_limit_bytes=4 << 20),
        cost_estimate=pl.CostEstimate(
            flops=width * tiles.size, bytes_accessed=tiles.size, transcendentals=0
        ),
    )(counts, cols, arrived, tiles)


def sums_kernel(vectors, image1, image2, sums):
    n = vectors.shape[0]
    first = jnp.concatenate([image1[...], vectors[...]], axis=0)
    second = jnp.concatenate([image2[...], image1[...]], axis=0)
    sums[:, : 2 * n] = nt_dot(image1[...], first, HIGHEST)
    sums[:, 2 * n :] = nt_dot(image2[...], second, HIGHEST)


def sums_of(vectors, image1, image2):
    n = vectors.shape[0]
    return pl.pallas_call(
        sums_kernel,
        out_shape=jax.ShapeDtypeStruct((n, 4 * n), F32),
        in_specs=[vmem()] * 3,
        out_specs=vmem(),
        compiler_params=pltpu.CompilerParams(vmem_limit_bytes=16 << 20),
    )(vectors, image1, image2)


def inverse_factors(grams):
    n = grams[0].shape[0]
    wide = 2 * n
    group = 8
    pieces = n // group
    sub = lax.broadcasted_iota(jnp.int32, (group, wide), 0)
    lane = lax.broadcasted_iota(jnp.int32, (group, wide), 1)

    def spread(row):
        return jnp.broadcast_to(row, (group, wide))

    held = []
    for a in grams:
        rows = []
        for r in range(pieces):
            eye = (lane == sub + (n + group * r)).astype(F32)[:, n:]
            rows.append(jnp.concatenate([a[group * r : group * (r + 1), :], eye], axis=1))
        held.append(rows)
    pivots = [[] for _ in grams]
    for k in range(pieces):
        columns = [
            [[spread(m[r][:, j : j + 1]) for r in range(k, pieces)] for j in range(group * k, group * (k + 1))]
            for m in held
        ]
        found = [jnp.ones((group, wide), F32) for _ in grams]
        for j in range(group):
            for p, m in enumerate(held):
                column = columns[p]
                pivot = spread(column[j][0][j : j + 1, :])
                found[p] = jnp.where(sub == j, pivot, found[p])
                row = spread(m[k][j : j + 1, :]) / pivot
                later = [spread(column[i][0][j : j + 1, :]) / pivot for i in range(j + 1, group)]
                for r in range(k, pieces):
                    factor = column[j][r - k]
                    if r == k:
                        factor = jnp.where(sub > j, factor, 0.0)
                    m[r] = m[r] - factor * row
                    for i in range(j + 1, group):
                        column[i][r - k] = column[i][r - k] - factor * later[i - j - 1]
        for p in range(len(grams)):
            pivots[p].append(found[p])
    return [
        jnp.concatenate(
            [(held[p][r] / jnp.sqrt(pivots[p][r]))[:, n:] for r in range(pieces)], axis=0
        )
        for p in range(len(grams))
    ]


def diagonal(a):
    n = a.shape[0]
    row = lax.broadcasted_iota(jnp.int32, (n, n), 0)
    lane = lax.broadcasted_iota(jnp.int32, (n, n), 1)
    return jnp.sum(jnp.where(row == lane, a, 0.0), axis=0, keepdims=True)


def in_range(d):
    return (jnp.min(d) > SMALL) & (jnp.max(d) < LARGE)


def factor_kernel(total_rows, sums, inverse2, rayleigh, good):
    n = inverse2.shape[0]
    scale = 1.0 / (total_rows**0.5)
    gram1, gram2 = [sums[:, i * n : (i + 1) * n] * (1.0 / total_rows) for i in (0, 2)]
    x1, x2 = inverse_factors([gram1, gram2])
    inverse2[...] = x2
    rayleigh[0] = sums[:, n : 2 * n].T * scale
    right = nt_dot(sums[:, 3 * n :].T, x1, HIGHEST)
    rayleigh[1] = jnp.dot(x1, right, precision=HIGHEST, preferred_element_type=F32) * scale
    d1 = diagonal(gram1)
    gain = jnp.sum(x1 * x1 * d1) * (1.0 / n)
    fine = in_range(d1) & in_range(diagonal(gram2)) & (gain < GAIN_LIMIT)
    good[0] = (fine & (jnp.max(jnp.abs(x2)) < LARGE)).astype(jnp.int32)


def factor(total_rows, sums):
    n = sums.shape[0]
    return pl.pallas_call(
        functools.partial(factor_kernel, total_rows),
        out_shape=(
            jax.ShapeDtypeStruct((n, n), F32),
            jax.ShapeDtypeStruct((2, n, n), F32),
            jax.ShapeDtypeStruct((1,), jnp.int32),
        ),
        in_specs=[vmem()],
        out_specs=(vmem(), vmem(), smem()),
    )(sums)


def sum_everywhere(value, devices):
    if devices & (devices - 1):
        return lax.psum(value, AXES)

    def from_peer(v, mask):
        return lax.ppermute(v, AXES, [(i, i ^ mask) for i in range(devices)])

    bits = devices.bit_length() - 1
    bit = 0
    if bits % 2:
        value = value + from_peer(value, 1)
        bit = 1
    while bit < bits:
        a, b = 1 << bit, 2 << bit
        value = (value + from_peer(value, a)) + (from_peer(value, b) + from_peer(value, a | b))
        bit += 2
    return value


def step_by_step(vectors, tiles, counts, tile_col, send_list):
    me = lax.axis_index(AXES)
    outgoing = lax.dynamic_index_in_dim(send_list, me, 0, keepdims=False).reshape(-1)
    devices = lax.axis_size(AXES)
    width, rows_here = vectors.shape
    blocks_here = counts.shape[0]
    tile_size = tiles.shape[1]
    depth = tiles.shape[0] // blocks_here
    total_rows = rows_here * devices
    live = jnp.arange(tiles.shape[0], dtype=jnp.int32) % depth < jnp.repeat(counts, depth)
    live = live.astype(F32)
    current = vectors
    rayleigh = []
    for step in range(ITERS):
        rounded = current.astype(BF16)
        own_blocks = rounded.reshape(width, blocks_here, tile_size).transpose(1, 0, 2)
        parcel = jnp.take(own_blocks, outgoing, axis=0)
        arrived = lax.all_to_all(parcel, AXES, split_axis=0, concat_axis=0, tiled=True)
        picked = jnp.take(arrived, tile_col, axis=0)
        prod = jnp.einsum("jrc,jkc->jkr", tiles, picked, preferred_element_type=F32)
        prod = prod * live[:, None, None]
        image = prod.reshape(blocks_here, depth, width, tile_size).sum(axis=1)
        image = image.transpose(1, 0, 2).reshape(width, rows_here)
        gram_part = jnp.dot(image, image.T, precision=HIGHEST)
        quotient_part = jnp.dot(current, image.T, precision=HIGHEST)
        gram, quotient = lax.psum((gram_part, quotient_part), AXES)
        gram = gram / total_rows
        rayleigh.append(quotient / jnp.sqrt(F32(total_rows)))
        lower = jnp.linalg.cholesky(gram)
        current = lax.linalg.triangular_solve(lower, image, left_side=True, lower=True)
    return current, jnp.stack(rayleigh)


def on_device(vectors, tiles, counts, tile_col, send_list):
    devices = lax.axis_size(AXES)
    total_rows = vectors.shape[1] * devices
    exchange = Exchange(devices, send_list, tiles.shape[1])
    cols = exchange.arrival(tile_col)
    arrived = exchange(vectors.astype(BF16), cols)
    image1, rounded = image_of((F32, BF16), counts, cols, arrived, tiles)
    (image2,) = image_of((F32,), counts, cols, exchange(rounded), tiles)
    sums = sum_everywhere(sums_of(vectors, image1, image2), devices)
    inverse2, rayleigh, good = factor(total_rows, sums)

    def fast():
        return jnp.dot(inverse2, image2, precision=HIGHEST), rayleigh

    def slow():
        return step_by_step(vectors, tiles, counts, tile_col, send_list)

    return lax.cond(good[0] > 0, fast, slow)


def solution(mesh):
    return jax.shard_map(
        on_device,
        mesh=mesh,
        in_specs=(
            P(None, AXES),
            P(AXES, None, None),
            P(AXES),
            P(AXES),
            P(),
        ),
        out_specs=(P(None, AXES), P()),
        check_vma=False,
    )
```

```python
import functools

import jax
import jax.numpy as jnp
from jax import lax
from jax.experimental import pallas as pl
from jax.experimental.pallas import tpu as pltpu
from jax.sharding import PartitionSpec as P

ITERS = 2
AXES = ("gx", "gy")
F32 = jnp.float32
BF16 = jnp.bfloat16
HIGHEST = lax.Precision.HIGHEST

GAIN_LIMIT = 1.5
SMALL, LARGE = 1e-25, 1e25
STEP = 4


def vmem():
    return pl.BlockSpec(memory_space=pltpu.VMEM)


def smem():
    return pl.BlockSpec(memory_space=pltpu.SMEM)


def nt_dot(a, b, precision=None):
    return lax.dot_general(
        a, b, (((1,), (1,)), ((), ())), precision=precision, preferred_element_type=F32
    )


def pack_kernel(outgoing, own, other, parcel):
    peers, rows, tile = parcel.shape
    width = own.shape[0]
    slots = rows // width // 2

    def one(p, carry):
        for i, source in enumerate((own, other)):
            for slot in range(slots):
                block = outgoing[(i * peers + p) * slots + slot]
                at = (i * slots + slot) * width
                parcel[p, at : at + width, :] = source[:, pl.ds(pl.multiple_of(block * tile, tile), tile)]
        return carry

    lax.fori_loop(0, peers, one, 0)


def pack(outgoing, own, other, peers, tile):
    width = own.shape[0]
    rows = outgoing.shape[0] // peers * width
    return pl.pallas_call(
        pack_kernel,
        out_shape=jax.ShapeDtypeStruct((peers, rows, tile), BF16),
        in_specs=[smem(), vmem(), vmem()],
        out_specs=vmem(),
        compiler_params=pltpu.CompilerParams(vmem_limit_bytes=4 << 20),
        cost_estimate=pl.CostEstimate(
            flops=5_000_000_000, bytes_accessed=32 << 20, transcendentals=0
        ),
    )(outgoing, own, other)


class Exchange:
    def __init__(self, devices, send_list, tile):
        assert devices >= 4 and devices & (devices - 1) == 0
        self.quarter = quarter = devices // 4
        self.peers = 2 * quarter
        self.swap = [(i, i ^ quarter) for i in range(devices)]
        self.groups = [
            [q * quarter + i for q in quarters for i in range(quarter)] for quarters in ((0, 3), (1, 2))
        ]
        self.tile = tile
        self.slots = send_list.shape[2]
        me = lax.axis_index(AXES)
        self.group = self.group_of(me)
        receivers = [self.group * quarter, (3 - self.group) * quarter]
        lists = [
            lax.dynamic_slice(send_list, (source, receiver, 0), (1, quarter, self.slots))
            for source in (me, me ^ quarter)
            for receiver in receivers
        ]
        self.outgoing = jnp.concatenate(lists).reshape(-1)

    def group_of(self, device):
        place = device // self.quarter
        return (place ^ (place >> 1)) & 1

    def arrival(self, tile_col):
        sender, slot = tile_col // self.slots, tile_col % self.slots
        far = self.group_of(sender) ^ self.group
        near = sender ^ (far * self.quarter)
        near = near // self.peers * self.quarter + near % self.quarter
        return (2 * near + far) * self.slots + slot

    def __call__(self, rounded, *ahead):
        other = lax.ppermute(rounded, AXES, self.swap)
        parcel = pack(self.outgoing, rounded, other, self.peers, self.tile)
        parcel, *ahead = lax.optimization_barrier((parcel, *ahead))
        arrived = lax.all_to_all(
            parcel, AXES, split_axis=0, concat_axis=0, axis_index_groups=self.groups, tiled=True
        )
        return (arrived.reshape(-1, rounded.shape[0], self.tile), *ahead)


def image_kernel(counts, cols, arrived, tiles, image, *rounded):
    blocks = counts.shape[0]
    depth = tiles.shape[0] // blocks
    tile = tiles.shape[1]
    width = arrived.shape[1]
    mxus = (0, 1)

    def push(b, t, register, mxu):
        pltpu.matmul_push_rhs(
            tiles[b * depth + t], staging_register=register, mxu_index=mxu, transpose=True
        )

    def block(b, t):
        found = arrived[cols[b * depth + t]]
        return jnp.where(t < counts[b], found, jnp.zeros_like(found))

    def run(*refs):
        sums = (refs[0:2], refs[2:4])
        spare = refs[4:6]
        for ref in refs:
            pltpu.matmul_pop(ref)

        def flush(b):
            first, second = sums[b % 2]
            value = pltpu.matmul_pop(first) + pltpu.matmul_pop(second)
            for ref in (image, *rounded):
                ref[:, b * tile : (b + 1) * tile] = value.astype(ref.dtype)

        for mxu in mxus:
            push(0, mxu, 0, mxu)
        for b in range(blocks):
            steps = (counts[b] + STEP - 1) // STEP

            def products(t, push_next):
                for mxu in mxus:
                    push(b, t + 2 + mxu, 1, mxu)
                for mxu in mxus:
                    pltpu.matmul_acc_lhs(sums[b % 2][mxu], block(b, t + mxu), load_staged_rhs=0)
                for mxu in mxus:
                    push_next(mxu)
                for mxu in mxus:
                    pltpu.matmul_acc_lhs(sums[b % 2][mxu], block(b, t + 2 + mxu), load_staged_rhs=1)

            def step(q, carry):
                products(q * STEP, lambda mxu: push(b, (q + 1) * STEP + mxu, 0, mxu))
                return carry

            lax.fori_loop(0, steps - 1, step, 0)
            products((steps - 1) * STEP, lambda mxu: push(min(b + 1, blocks - 1), mxu, 0, mxu))
            if b:
                flush(b - 1)
        for mxu in mxus:
            pltpu.matmul_acc_lhs(spare[mxu], jnp.zeros((16, tile), BF16), load_staged_rhs=0)
        flush(blocks - 1)
        for ref in spare:
            pltpu.matmul_pop(ref)

    pl.run_scoped(
        run,
        *[pltpu.ACC(mxu)((width, tile), F32) for mxu in mxus + mxus],
        *[pltpu.ACC(mxu)((16, tile), F32) for mxu in mxus],
    )


def image_of(kinds, counts, cols, arrived, tiles):
    width, tile = arrived.shape[1:]
    blocks = counts.shape[0]
    assert tile == 256 and width % 16 == 0 and width <= 256
    assert tiles.shape[0] % (blocks * STEP) == 0
    grant = (4 if 16 * arrived.size <= tiles.size else 24) << 20
    return pl.pallas_call(
        image_kernel,
        out_shape=[jax.ShapeDtypeStruct((width, blocks * tile), kind) for kind in kinds],
        in_specs=[smem(), smem(), vmem(), vmem()],
        out_specs=[vmem()] * len(kinds),
        compiler_params=pltpu.CompilerParams(vmem_limit_bytes=grant),
        cost_estimate=pl.CostEstimate(
            flops=width * tiles.size, bytes_accessed=tiles.size, transcendentals=0
        ),
    )(counts, cols, arrived, tiles)


def first_sums_kernel(vectors, image, sums):
    sums[...] = nt_dot(image[...], jnp.concatenate([image[...], vectors[...]], axis=0), HIGHEST)


def first_sums(vectors, image):
    n = vectors.shape[0]
    return pl.pallas_call(
        first_sums_kernel,
        out_shape=jax.ShapeDtypeStruct((n, 2 * n), F32),
        in_specs=[vmem()] * 2,
        out_specs=vmem(),
        compiler_params=pltpu.CompilerParams(vmem_limit_bytes=4 << 20),
    )(vectors, image)


def halves_kernel(odd, sums1, image1, image2, kept, given):
    sums2 = nt_dot(image2[...], jnp.concatenate([image2[...], image1[...]], axis=0), HIGHEST)
    for when, mine, other in ((0, sums1, None), (1, None, sums1)):

        @pl.when(odd[0] == when)
        def _():
            kept[...] = sums2 if mine is None else mine[...]
            given[...] = sums2 if other is None else other[...]


def halves(odd, sums1, image1, image2):
    shape = jax.ShapeDtypeStruct(sums1.shape, F32)
    return pl.pallas_call(
        halves_kernel,
        out_shape=(shape, shape),
        in_specs=[smem()] + [vmem()] * 3,
        out_specs=(vmem(), vmem()),
        compiler_params=pltpu.CompilerParams(vmem_limit_bytes=4 << 20),
    )(odd, sums1, image1, image2)


def inverse_factors(grams):
    n = grams[0].shape[0]
    wide = 2 * n
    group = 8
    pieces = n // group
    sub = lax.broadcasted_iota(jnp.int32, (group, wide), 0)
    lane = lax.broadcasted_iota(jnp.int32, (group, wide), 1)

    def spread(row):
        return jnp.broadcast_to(row, (group, wide))

    held = []
    for a in grams:
        rows = []
        for r in range(pieces):
            eye = (lane == sub + (n + group * r)).astype(F32)[:, n:]
            rows.append(jnp.concatenate([a[group * r : group * (r + 1), :], eye], axis=1))
        held.append(rows)
    pivots = [[] for _ in grams]
    for k in range(pieces):
        columns = [
            [[spread(m[r][:, j : j + 1]) for r in range(k, pieces)] for j in range(group * k, group * (k + 1))]
            for m in held
        ]
        found = [jnp.ones((group, wide), F32) for _ in grams]
        for j in range(group):
            for p, m in enumerate(held):
                column = columns[p]
                pivot = spread(column[j][0][j : j + 1, :])
                found[p] = jnp.where(sub == j, pivot, found[p])
                row = spread(m[k][j : j + 1, :]) / pivot
                later = [spread(column[i][0][j : j + 1, :]) / pivot for i in range(j + 1, group)]
                for r in range(k, pieces):
                    factor = column[j][r - k]
                    if r == k:
                        factor = jnp.where(sub > j, factor, 0.0)
                    m[r] = m[r] - factor * row
                    for i in range(j + 1, group):
                        column[i][r - k] = column[i][r - k] - factor * later[i - j - 1]
        for p in range(len(grams)):
            pivots[p].append(found[p])
    return [
        jnp.concatenate(
            [(held[p][r] / jnp.sqrt(pivots[p][r]))[:, n:] for r in range(pieces)], axis=0
        )
        for p in range(len(grams))
    ]


def diagonal(a):
    n = a.shape[0]
    row = lax.broadcasted_iota(jnp.int32, (n, n), 0)
    lane = lax.broadcasted_iota(jnp.int32, (n, n), 1)
    return jnp.sum(jnp.where(row == lane, a, 0.0), axis=0, keepdims=True)


def in_range(d):
    return (jnp.min(d) > SMALL) & (jnp.max(d) < LARGE)


def factor_kernel(total_rows, odd, kept, received, inverse2, rayleigh, good):
    n = inverse2.shape[0]
    scale = 1.0 / (total_rows**0.5)
    sums1 = jnp.where(odd[0] == 0, kept[...], received[...])
    sums2 = jnp.where(odd[0] == 0, received[...], kept[...])
    gram1, gram2 = [sums[:, :n] * (1.0 / total_rows) for sums in (sums1, sums2)]
    x1, x2 = inverse_factors([gram1, gram2])
    inverse2[...] = x2
    rayleigh[0] = sums1[:, n:].T * scale
    right = nt_dot(sums2[:, n:].T, x1, HIGHEST)
    rayleigh[1] = jnp.dot(x1, right, precision=HIGHEST, preferred_element_type=F32) * scale
    d1 = diagonal(gram1)
    gain = jnp.sum(x1 * x1 * d1) * (1.0 / n)
    fine = in_range(d1) & in_range(diagonal(gram2)) & (gain < GAIN_LIMIT)
    good[0] = (fine & (jnp.max(jnp.abs(x2)) < LARGE)).astype(jnp.int32)


def factor(total_rows, odd, kept, received):
    n = kept.shape[0]
    return pl.pallas_call(
        functools.partial(factor_kernel, total_rows),
        out_shape=(
            jax.ShapeDtypeStruct((n, n), F32),
            jax.ShapeDtypeStruct((2, n, n), F32),
            jax.ShapeDtypeStruct((1,), jnp.int32),
        ),
        in_specs=[smem(), vmem(), vmem()],
        out_specs=(vmem(), vmem(), smem()),
        compiler_params=pltpu.CompilerParams(vmem_limit_bytes=8 << 20),
    )(odd, kept, received)


def from_peer(value, mask):
    devices = lax.axis_size(AXES)
    return lax.ppermute(value, AXES, [(i, i ^ mask) for i in range(devices)])


def sum_halves(kept, given):
    kept = kept + from_peer(given, 1)
    bit, last = 2, lax.axis_size(AXES)
    if last.bit_length() % 2 == 1:
        kept = kept + from_peer(kept, bit)
        bit *= 2
    while bit < last:
        near, far = from_peer(kept, bit), from_peer(kept, 2 * bit)
        kept = (kept + near) + (far + from_peer(kept, 3 * bit))
        bit *= 4
    return kept, from_peer(kept, 1)


def step_by_step(vectors, tiles, counts, tile_col, send_list):
    me = lax.axis_index(AXES)
    outgoing = lax.dynamic_index_in_dim(send_list, me, 0, keepdims=False).reshape(-1)
    devices = lax.axis_size(AXES)
    width, rows_here = vectors.shape
    blocks_here = counts.shape[0]
    tile_size = tiles.shape[1]
    depth = tiles.shape[0] // blocks_here
    total_rows = rows_here * devices
    live = jnp.arange(tiles.shape[0], dtype=jnp.int32) % depth < jnp.repeat(counts, depth)
    live = live.astype(F32)
    current = vectors
    rayleigh = []
    for step in range(ITERS):
        rounded = current.astype(BF16)
        own_blocks = rounded.reshape(width, blocks_here, tile_size).transpose(1, 0, 2)
        parcel = jnp.take(own_blocks, outgoing, axis=0)
        arrived = lax.all_to_all(parcel, AXES, split_axis=0, concat_axis=0, tiled=True)
        picked = jnp.take(arrived, tile_col, axis=0)
        prod = jnp.einsum("jrc,jkc->jkr", tiles, picked, preferred_element_type=F32)
        prod = prod * live[:, None, None]
        image = prod.reshape(blocks_here, depth, width, tile_size).sum(axis=1)
        image = image.transpose(1, 0, 2).reshape(width, rows_here)
        gram_part = jnp.dot(image, image.T, precision=HIGHEST)
        quotient_part = jnp.dot(current, image.T, precision=HIGHEST)
        gram, quotient = lax.psum((gram_part, quotient_part), AXES)
        gram = gram / total_rows
        rayleigh.append(quotient / jnp.sqrt(F32(total_rows)))
        lower = jnp.linalg.cholesky(gram)
        current = lax.linalg.triangular_solve(lower, image, left_side=True, lower=True)
    return current, jnp.stack(rayleigh)


def on_device(vectors, tiles, counts, tile_col, send_list):
    devices = lax.axis_size(AXES)
    total_rows = vectors.shape[1] * devices
    exchange = Exchange(devices, send_list, tiles.shape[1])
    odd = (lax.axis_index(AXES) & 1).reshape(1)
    arrived, cols, odd = exchange(vectors.astype(BF16), exchange.arrival(tile_col), odd)
    image1, rounded = image_of((F32, BF16), counts, cols, arrived, tiles)
    arrived, sums1 = exchange(rounded, first_sums(vectors, image1))
    (image2,) = image_of((F32,), counts, cols, arrived, tiles)
    kept, received = sum_halves(*halves(odd, sums1, image1, image2))
    inverse2, rayleigh, good = factor(total_rows, odd, kept, received)

    def fast():
        return jnp.dot(inverse2, image2, precision=HIGHEST), rayleigh

    def slow():
        return step_by_step(vectors, tiles, counts, tile_col, send_list)

    return lax.cond(good[0] > 0, fast, slow)


def solution(mesh):
    return jax.shard_map(
        on_device,
        mesh=mesh,
        in_specs=(
            P(None, AXES),
            P(AXES, None, None),
            P(AXES),
            P(AXES),
            P(),
        ),
        out_specs=(P(None, AXES), P()),
        check_vma=False,
    )
```

```python
import functools

import jax
import jax.numpy as jnp
from jax import lax
from jax.experimental import pallas as pl
from jax.experimental.pallas import tpu as pltpu
from jax.sharding import PartitionSpec as P

ITERS = 2
AXES = ("gx", "gy")
F32 = jnp.float32
BF16 = jnp.bfloat16
HIGHEST = lax.Precision.HIGHEST

GAIN_LIMIT = 1.5
SMALL, LARGE = 1e-25, 1e25
STEP = 4


def vmem():
    return pl.BlockSpec(memory_space=pltpu.VMEM)


def smem():
    return pl.BlockSpec(memory_space=pltpu.SMEM)


def nt_dot(a, b, precision=None):
    return lax.dot_general(
        a, b, (((1,), (1,)), ((), ())), precision=precision, preferred_element_type=F32
    )


def pack_kernel(outgoing, own, other, parcel):
    peers, rows, tile = parcel.shape
    width = own.shape[0]
    slots = rows // width // 2

    def one(p, carry):
        for i, source in enumerate((own, other)):
            for slot in range(slots):
                block = outgoing[(i * peers + p) * slots + slot]
                at = (i * slots + slot) * width
                parcel[p, at : at + width, :] = source[:, pl.ds(pl.multiple_of(block * tile, tile), tile)]
        return carry

    lax.fori_loop(0, peers, one, 0)


def pack(outgoing, own, other, peers, tile):
    width = own.shape[0]
    rows = outgoing.shape[0] // peers * width
    return pl.pallas_call(
        pack_kernel,
        out_shape=jax.ShapeDtypeStruct((peers, rows, tile), BF16),
        in_specs=[smem(), vmem(), vmem()],
        out_specs=vmem(),
        compiler_params=pltpu.CompilerParams(vmem_limit_bytes=4 << 20),
        cost_estimate=pl.CostEstimate(
            flops=5_000_000_000, bytes_accessed=32 << 20, transcendentals=0
        ),
    )(outgoing, own, other)


class Exchange:
    def __init__(self, devices, send_list, tile):
        assert devices >= 4 and devices & (devices - 1) == 0
        self.peers = half = devices // 2
        self.swap = [(i, i ^ half) for i in range(devices)]
        self.groups = [list(range(half)), list(range(half, devices))]
        self.tile = tile
        self.slots = send_list.shape[2]
        me = lax.axis_index(AXES)
        self.side = (me >= half).astype(jnp.int32)
        lists = [
            lax.dynamic_slice(send_list, (source, self.side * half, 0), (1, half, self.slots))
            for source in (me, me ^ half)
        ]
        self.outgoing = jnp.concatenate(lists).reshape(-1)

    def arrival(self, tile_col):
        sender, slot = tile_col // self.slots, tile_col % self.slots
        far = (sender >= self.peers).astype(jnp.int32) ^ self.side
        return (2 * (sender % self.peers) + far) * self.slots + slot

    def __call__(self, rounded, *ahead):
        other = lax.ppermute(rounded, AXES, self.swap)
        parcel = pack(self.outgoing, rounded, other, self.peers, self.tile)
        parcel, *ahead = lax.optimization_barrier((parcel, *ahead))
        arrived = lax.all_to_all(
            parcel, AXES, split_axis=0, concat_axis=0, axis_index_groups=self.groups, tiled=True
        )
        return (arrived.reshape(-1, rounded.shape[0], self.tile), *ahead)


def image_kernel(counts, cols, arrived, tiles, image, *rounded):
    blocks = counts.shape[0]
    depth = tiles.shape[0] // blocks
    tile = tiles.shape[1]
    width = arrived.shape[1]
    mxus = (0, 1)

    def push(b, t, register, mxu):
        pltpu.matmul_push_rhs(
            tiles[b * depth + t], staging_register=register, mxu_index=mxu, transpose=True
        )

    def block(b, t):
        found = arrived[cols[b * depth + t]]
        return jnp.where(t < counts[b], found, jnp.zeros_like(found))

    def run(*refs):
        sums = (refs[0:2], refs[2:4])
        spare = refs[4:6]
        for ref in refs:
            pltpu.matmul_pop(ref)

        def flush(b):
            first, second = sums[b % 2]
            value = pltpu.matmul_pop(first) + pltpu.matmul_pop(second)
            for ref in (image, *rounded):
                ref[:, b * tile : (b + 1) * tile] = value.astype(ref.dtype)

        for mxu in mxus:
            push(0, mxu, 0, mxu)
        for b in range(blocks):
            steps = (counts[b] + STEP - 1) // STEP

            def products(t, push_next):
                for mxu in mxus:
                    push(b, t + 2 + mxu, 1, mxu)
                for mxu in mxus:
                    pltpu.matmul_acc_lhs(sums[b % 2][mxu], block(b, t + mxu), load_staged_rhs=0)
                for mxu in mxus:
                    push_next(mxu)
                for mxu in mxus:
                    pltpu.matmul_acc_lhs(sums[b % 2][mxu], block(b, t + 2 + mxu), load_staged_rhs=1)

            def step(q, carry):
                products(q * STEP, lambda mxu: push(b, (q + 1) * STEP + mxu, 0, mxu))
                return carry

            lax.fori_loop(0, steps - 1, step, 0)
            products((steps - 1) * STEP, lambda mxu: push(min(b + 1, blocks - 1), mxu, 0, mxu))
            if b:
                flush(b - 1)
        for mxu in mxus:
            pltpu.matmul_acc_lhs(spare[mxu], jnp.zeros((16, tile), BF16), load_staged_rhs=0)
        flush(blocks - 1)
        for ref in spare:
            pltpu.matmul_pop(ref)

    pl.run_scoped(
        run,
        *[pltpu.ACC(mxu)((width, tile), F32) for mxu in mxus + mxus],
        *[pltpu.ACC(mxu)((16, tile), F32) for mxu in mxus],
    )


def image_of(kinds, counts, cols, arrived, tiles):
    width, tile = arrived.shape[1:]
    blocks = counts.shape[0]
    assert tile == 256 and width % 16 == 0 and width <= 256
    assert tiles.shape[0] % (blocks * STEP) == 0
    grant = (4 if 16 * arrived.size <= tiles.size else 24) << 20
    return pl.pallas_call(
        image_kernel,
        out_shape=[jax.ShapeDtypeStruct((width, blocks * tile), kind) for kind in kinds],
        in_specs=[smem(), smem(), vmem(), vmem()],
        out_specs=[vmem()] * len(kinds),
        compiler_params=pltpu.CompilerParams(vmem_limit_bytes=grant),
        cost_estimate=pl.CostEstimate(
            flops=width * tiles.size, bytes_accessed=tiles.size, transcendentals=0
        ),
    )(counts, cols, arrived, tiles)


def first_sums_kernel(vectors, image, sums):
    sums[...] = nt_dot(image[...], jnp.concatenate([image[...], vectors[...]], axis=0), HIGHEST)


def first_sums(vectors, image):
    n = vectors.shape[0]
    return pl.pallas_call(
        first_sums_kernel,
        out_shape=jax.ShapeDtypeStruct((n, 2 * n), F32),
        in_specs=[vmem()] * 2,
        out_specs=vmem(),
        compiler_params=pltpu.CompilerParams(vmem_limit_bytes=4 << 20),
    )(vectors, image)


def halves_kernel(odd, sums1, image1, image2, kept, given):
    sums2 = nt_dot(image2[...], jnp.concatenate([image2[...], image1[...]], axis=0), HIGHEST)
    for when, mine, other in ((0, sums1, None), (1, None, sums1)):

        @pl.when(odd[0] == when)
        def _():
            kept[...] = sums2 if mine is None else mine[...]
            given[...] = sums2 if other is None else other[...]


def halves(odd, sums1, image1, image2):
    shape = jax.ShapeDtypeStruct(sums1.shape, F32)
    return pl.pallas_call(
        halves_kernel,
        out_shape=(shape, shape),
        in_specs=[smem()] + [vmem()] * 3,
        out_specs=(vmem(), vmem()),
        compiler_params=pltpu.CompilerParams(vmem_limit_bytes=4 << 20),
    )(odd, sums1, image1, image2)


def inverse_factors(grams):
    n = grams[0].shape[0]
    wide = 2 * n
    group = 8
    pieces = n // group
    sub = lax.broadcasted_iota(jnp.int32, (group, wide), 0)
    lane = lax.broadcasted_iota(jnp.int32, (group, wide), 1)

    def spread(row):
        return jnp.broadcast_to(row, (group, wide))

    held = []
    for a in grams:
        rows = []
        for r in range(pieces):
            eye = (lane == sub + (n + group * r)).astype(F32)[:, n:]
            rows.append(jnp.concatenate([a[group * r : group * (r + 1), :], eye], axis=1))
        held.append(rows)
    pivots = [[] for _ in grams]
    for k in range(pieces):
        columns = [
            [[spread(m[r][:, j : j + 1]) for r in range(k, pieces)] for j in range(group * k, group * (k + 1))]
            for m in held
        ]
        found = [jnp.ones((group, wide), F32) for _ in grams]
        for j in range(group):
            for p, m in enumerate(held):
                column = columns[p]
                pivot = spread(column[j][0][j : j + 1, :])
                found[p] = jnp.where(sub == j, pivot, found[p])
                row = spread(m[k][j : j + 1, :]) / pivot
                later = [spread(column[i][0][j : j + 1, :]) / pivot for i in range(j + 1, group)]
                for r in range(k, pieces):
                    factor = column[j][r - k]
                    if r == k:
                        factor = jnp.where(sub > j, factor, 0.0)
                    m[r] = m[r] - factor * row
                    for i in range(j + 1, group):
                        column[i][r - k] = column[i][r - k] - factor * later[i - j - 1]
        for p in range(len(grams)):
            pivots[p].append(found[p])
    return [
        jnp.concatenate(
            [(held[p][r] / jnp.sqrt(pivots[p][r]))[:, n:] for r in range(pieces)], axis=0
        )
        for p in range(len(grams))
    ]


def diagonal(a):
    n = a.shape[0]
    row = lax.broadcasted_iota(jnp.int32, (n, n), 0)
    lane = lax.broadcasted_iota(jnp.int32, (n, n), 1)
    return jnp.sum(jnp.where(row == lane, a, 0.0), axis=0, keepdims=True)


def in_range(d):
    return (jnp.min(d) > SMALL) & (jnp.max(d) < LARGE)


def factor_kernel(total_rows, odd, kept, received, inverse2, rayleigh, good):
    n = inverse2.shape[0]
    scale = 1.0 / (total_rows**0.5)
    sums1 = jnp.where(odd[0] == 0, kept[...], received[...])
    sums2 = jnp.where(odd[0] == 0, received[...], kept[...])
    gram1, gram2 = [sums[:, :n] * (1.0 / total_rows) for sums in (sums1, sums2)]
    x1, x2 = inverse_factors([gram1, gram2])
    inverse2[...] = x2
    rayleigh[0] = sums1[:, n:].T * scale
    right = nt_dot(sums2[:, n:].T, x1, HIGHEST)
    rayleigh[1] = jnp.dot(x1, right, precision=HIGHEST, preferred_element_type=F32) * scale
    d1 = diagonal(gram1)
    gain = jnp.sum(x1 * x1 * d1) * (1.0 / n)
    fine = in_range(d1) & in_range(diagonal(gram2)) & (gain < GAIN_LIMIT)
    good[0] = (fine & (jnp.max(jnp.abs(x2)) < LARGE)).astype(jnp.int32)


def factor(total_rows, odd, kept, received):
    n = kept.shape[0]
    return pl.pallas_call(
        functools.partial(factor_kernel, total_rows),
        out_shape=(
            jax.ShapeDtypeStruct((n, n), F32),
            jax.ShapeDtypeStruct((2, n, n), F32),
            jax.ShapeDtypeStruct((1,), jnp.int32),
        ),
        in_specs=[smem(), vmem(), vmem()],
        out_specs=(vmem(), vmem(), smem()),
        compiler_params=pltpu.CompilerParams(vmem_limit_bytes=8 << 20),
    )(odd, kept, received)


def from_peer(value, mask):
    devices = lax.axis_size(AXES)
    return lax.ppermute(value, AXES, [(i, i ^ mask) for i in range(devices)])


def sum_halves(kept, given):
    kept = kept + from_peer(given, 1)
    bit, last = 2, lax.axis_size(AXES)
    if last.bit_length() % 2 == 1:
        kept = kept + from_peer(kept, bit)
        bit *= 2
    while bit < last:
        near, far = from_peer(kept, bit), from_peer(kept, 2 * bit)
        kept = (kept + near) + (far + from_peer(kept, 3 * bit))
        bit *= 4
    return kept, from_peer(kept, 1)


def step_by_step(vectors, tiles, counts, tile_col, send_list):
    me = lax.axis_index(AXES)
    outgoing = lax.dynamic_index_in_dim(send_list, me, 0, keepdims=False).reshape(-1)
    devices = lax.axis_size(AXES)
    width, rows_here = vectors.shape
    blocks_here = counts.shape[0]
    tile_size = tiles.shape[1]
    depth = tiles.shape[0] // blocks_here
    total_rows = rows_here * devices
    live = jnp.arange(tiles.shape[0], dtype=jnp.int32) % depth < jnp.repeat(counts, depth)
    live = live.astype(F32)
    current = vectors
    rayleigh = []
    for step in range(ITERS):
        rounded = current.astype(BF16)
        own_blocks = rounded.reshape(width, blocks_here, tile_size).transpose(1, 0, 2)
        parcel = jnp.take(own_blocks, outgoing, axis=0)
        arrived = lax.all_to_all(parcel, AXES, split_axis=0, concat_axis=0, tiled=True)
        picked = jnp.take(arrived, tile_col, axis=0)
        prod = jnp.einsum("jrc,jkc->jkr", tiles, picked, preferred_element_type=F32)
        prod = prod * live[:, None, None]
        image = prod.reshape(blocks_here, depth, width, tile_size).sum(axis=1)
        image = image.transpose(1, 0, 2).reshape(width, rows_here)
        gram_part = jnp.dot(image, image.T, precision=HIGHEST)
        quotient_part = jnp.dot(current, image.T, precision=HIGHEST)
        gram, quotient = lax.psum((gram_part, quotient_part), AXES)
        gram = gram / total_rows
        rayleigh.append(quotient / jnp.sqrt(F32(total_rows)))
        lower = jnp.linalg.cholesky(gram)
        current = lax.linalg.triangular_solve(lower, image, left_side=True, lower=True)
    return current, jnp.stack(rayleigh)


def on_device(vectors, tiles, counts, tile_col, send_list):
    devices = lax.axis_size(AXES)
    total_rows = vectors.shape[1] * devices
    exchange = Exchange(devices, send_list, tiles.shape[1])
    odd = (lax.axis_index(AXES) & 1).reshape(1)
    arrived, cols, odd = exchange(vectors.astype(BF16), exchange.arrival(tile_col), odd)
    image1, rounded = image_of((F32, BF16), counts, cols, arrived, tiles)
    arrived, sums1 = exchange(rounded, first_sums(vectors, image1))
    (image2,) = image_of((F32,), counts, cols, arrived, tiles)
    kept, received = sum_halves(*halves(odd, sums1, image1, image2))
    inverse2, rayleigh, good = factor(total_rows, odd, kept, received)

    def fast():
        return jnp.dot(inverse2, image2, precision=HIGHEST), rayleigh

    def slow():
        return step_by_step(vectors, tiles, counts, tile_col, send_list)

    return lax.cond(good[0] > 0, fast, slow)


def solution(mesh):
    return jax.shard_map(
        on_device,
        mesh=mesh,
        in_specs=(
            P(None, AXES),
            P(AXES, None, None),
            P(AXES),
            P(AXES),
            P(),
        ),
        out_specs=(P(None, AXES), P()),
        check_vma=False,
    )
```

```python
import functools

import jax
import jax.numpy as jnp
from jax import lax
from jax.experimental import pallas as pl
from jax.experimental.pallas import tpu as pltpu
from jax.sharding import PartitionSpec as P

ITERS = 2
AXES = ("gx", "gy")
F32 = jnp.float32
BF16 = jnp.bfloat16
HIGHEST = lax.Precision.HIGHEST

GAIN_LIMIT = 1.5
SMALL, LARGE = 1e-25, 1e25
STEP = 4


def vmem():
    return pl.BlockSpec(memory_space=pltpu.VMEM)


def smem():
    return pl.BlockSpec(memory_space=pltpu.SMEM)


def nt_dot(a, b, precision=None):
    return lax.dot_general(
        a, b, (((1,), (1,)), ((), ())), precision=precision, preferred_element_type=F32
    )


def pack_kernel(outgoing, own, other, parcel):
    peers, rows, tile = parcel.shape
    width = own.shape[0]
    slots = rows // width // 2

    def one(p, carry):
        for i, source in enumerate((own, other)):
            for slot in range(slots):
                block = outgoing[(i * peers + p) * slots + slot]
                at = (i * slots + slot) * width
                parcel[p, at : at + width, :] = source[:, pl.ds(pl.multiple_of(block * tile, tile), tile)]
        return carry

    lax.fori_loop(0, peers, one, 0, unroll=8)


def pack(outgoing, own, other, peers, tile):
    width = own.shape[0]
    rows = outgoing.shape[0] // peers * width
    return pl.pallas_call(
        pack_kernel,
        out_shape=jax.ShapeDtypeStruct((peers, rows, tile), BF16),
        in_specs=[smem(), vmem(), vmem()],
        out_specs=vmem(),
        compiler_params=pltpu.CompilerParams(vmem_limit_bytes=4 << 20),
        cost_estimate=pl.CostEstimate(
            flops=5_000_000_000, bytes_accessed=32 << 20, transcendentals=0
        ),
    )(outgoing, own, other)


class Exchange:
    def __init__(self, devices, send_list, tile):
        assert devices >= 4 and devices & (devices - 1) == 0
        self.peers = half = devices // 2
        self.swap = [(i, i ^ half) for i in range(devices)]
        self.groups = [list(range(half)), list(range(half, devices))]
        self.tile = tile
        self.slots = send_list.shape[2]
        me = lax.axis_index(AXES)
        self.side = (me >= half).astype(jnp.int32)
        lists = [
            lax.dynamic_slice(send_list, (source, self.side * half, 0), (1, half, self.slots))
            for source in (me, me ^ half)
        ]
        self.outgoing = jnp.concatenate(lists).reshape(-1)

    def arrival(self, tile_col):
        sender, slot = tile_col // self.slots, tile_col % self.slots
        far = (sender >= self.peers).astype(jnp.int32) ^ self.side
        return (2 * (sender % self.peers) + far) * self.slots + slot

    def __call__(self, rounded, *ahead):
        other = lax.ppermute(rounded, AXES, self.swap)
        parcel = pack(self.outgoing, rounded, other, self.peers, self.tile)
        parcel, *ahead = lax.optimization_barrier((parcel, *ahead))
        arrived = lax.all_to_all(
            parcel, AXES, split_axis=0, concat_axis=0, axis_index_groups=self.groups, tiled=True
        )
        return (arrived.reshape(-1, rounded.shape[0], self.tile), *ahead)


def image_kernel(counts, cols, arrived, tiles, image, *rounded):
    blocks = counts.shape[0]
    depth = tiles.shape[0] // blocks
    tile = tiles.shape[1]
    width = arrived.shape[1]
    mxus = (0, 1)

    def push(b, t, register, mxu):
        pltpu.matmul_push_rhs(
            tiles[b * depth + t], staging_register=register, mxu_index=mxu, transpose=True
        )

    def block(b, t):
        found = arrived[cols[b * depth + t]]
        return jnp.where(t < counts[b], found, jnp.zeros_like(found))

    def run(*refs):
        sums = (refs[0:2], refs[2:4])
        spare = refs[4:6]
        for ref in refs:
            pltpu.matmul_pop(ref)

        def flush(b):
            first, second = sums[b % 2]
            value = pltpu.matmul_pop(first) + pltpu.matmul_pop(second)
            for ref in (image, *rounded):
                ref[:, b * tile : (b + 1) * tile] = value.astype(ref.dtype)

        for mxu in mxus:
            push(0, mxu, 0, mxu)
        for b in range(blocks):
            steps = (counts[b] + STEP - 1) // STEP

            def products(t, push_next):
                for mxu in mxus:
                    push(b, t + 2 + mxu, 1, mxu)
                for mxu in mxus:
                    pltpu.matmul_acc_lhs(sums[b % 2][mxu], block(b, t + mxu), load_staged_rhs=0)
                for mxu in mxus:
                    push_next(mxu)
                for mxu in mxus:
                    pltpu.matmul_acc_lhs(sums[b % 2][mxu], block(b, t + 2 + mxu), load_staged_rhs=1)

            def step(q, carry):
                products(q * STEP, lambda mxu: push(b, (q + 1) * STEP + mxu, 0, mxu))
                return carry

            lax.fori_loop(0, steps - 1, step, 0)
            products((steps - 1) * STEP, lambda mxu: push(min(b + 1, blocks - 1), mxu, 0, mxu))
            if b:
                flush(b - 1)
        for mxu in mxus:
            pltpu.matmul_acc_lhs(spare[mxu], jnp.zeros((16, tile), BF16), load_staged_rhs=0)
        flush(blocks - 1)
        for ref in spare:
            pltpu.matmul_pop(ref)

    pl.run_scoped(
        run,
        *[pltpu.ACC(mxu)((width, tile), F32) for mxu in mxus + mxus],
        *[pltpu.ACC(mxu)((16, tile), F32) for mxu in mxus],
    )


def image_of(kinds, counts, cols, arrived, tiles):
    width, tile = arrived.shape[1:]
    blocks = counts.shape[0]
    assert tile == 256 and width % 16 == 0 and width <= 256
    assert tiles.shape[0] % (blocks * STEP) == 0
    grant = (4 if 16 * arrived.size <= tiles.size else 24) << 20
    return pl.pallas_call(
        image_kernel,
        out_shape=[jax.ShapeDtypeStruct((width, blocks * tile), kind) for kind in kinds],
        in_specs=[smem(), smem(), vmem(), vmem()],
        out_specs=[vmem()] * len(kinds),
        compiler_params=pltpu.CompilerParams(vmem_limit_bytes=grant),
        cost_estimate=pl.CostEstimate(
            flops=width * tiles.size, bytes_accessed=tiles.size, transcendentals=0
        ),
    )(counts, cols, arrived, tiles)


def first_sums_kernel(vectors, image, sums):
    sums[...] = nt_dot(image[...], jnp.concatenate([image[...], vectors[...]], axis=0), HIGHEST)


def first_sums(vectors, image):
    n = vectors.shape[0]
    return pl.pallas_call(
        first_sums_kernel,
        out_shape=jax.ShapeDtypeStruct((n, 2 * n), F32),
        in_specs=[vmem()] * 2,
        out_specs=vmem(),
        compiler_params=pltpu.CompilerParams(vmem_limit_bytes=4 << 20),
    )(vectors, image)


def halves_kernel(odd, sums1, image1, image2, kept, given):
    sums2 = nt_dot(image2[...], jnp.concatenate([image2[...], image1[...]], axis=0), HIGHEST)
    for when, mine, other in ((0, sums1, None), (1, None, sums1)):

        @pl.when(odd[0] == when)
        def _():
            kept[...] = sums2 if mine is None else mine[...]
            given[...] = sums2 if other is None else other[...]


def halves(odd, sums1, image1, image2):
    shape = jax.ShapeDtypeStruct(sums1.shape, F32)
    return pl.pallas_call(
        halves_kernel,
        out_shape=(shape, shape),
        in_specs=[smem()] + [vmem()] * 3,
        out_specs=(vmem(), vmem()),
        compiler_params=pltpu.CompilerParams(vmem_limit_bytes=4 << 20),
    )(odd, sums1, image1, image2)


def inverse_factors(grams):
    n = grams[0].shape[0]
    wide = 2 * n
    group = 8
    pieces = n // group
    sub = lax.broadcasted_iota(jnp.int32, (group, wide), 0)
    lane = lax.broadcasted_iota(jnp.int32, (group, wide), 1)

    def spread(row):
        return jnp.broadcast_to(row, (group, wide))

    held = []
    for a in grams:
        rows = []
        for r in range(pieces):
            eye = (lane == sub + (n + group * r)).astype(F32)[:, n:]
            rows.append(jnp.concatenate([a[group * r : group * (r + 1), :], eye], axis=1))
        held.append(rows)
    pivots = [[] for _ in grams]
    for k in range(pieces):
        columns = [
            [[spread(m[r][:, j : j + 1]) for r in range(k, pieces)] for j in range(group * k, group * (k + 1))]
            for m in held
        ]
        found = [jnp.ones((group, wide), F32) for _ in grams]
        for j in range(group):
            for p, m in enumerate(held):
                column = columns[p]
                pivot = spread(column[j][0][j : j + 1, :])
                found[p] = jnp.where(sub == j, pivot, found[p])
                scale = 1.0 / pivot
                row = spread(m[k][j : j + 1, :])
                later = [spread(column[i][0][j : j + 1, :]) for i in range(j + 1, group)]
                for r in range(k, pieces):
                    factor = column[j][r - k] * scale
                    if r == k:
                        factor = jnp.where(sub > j, factor, 0.0)
                    m[r] = m[r] - factor * row
                    for i in range(j + 1, group):
                        column[i][r - k] = column[i][r - k] - factor * later[i - j - 1]
        for p in range(len(grams)):
            pivots[p].append(found[p])
    return [
        jnp.concatenate(
            [(held[p][r] / jnp.sqrt(pivots[p][r]))[:, n:] for r in range(pieces)], axis=0
        )
        for p in range(len(grams))
    ]


def diagonal(a):
    n = a.shape[0]
    row = lax.broadcasted_iota(jnp.int32, (n, n), 0)
    lane = lax.broadcasted_iota(jnp.int32, (n, n), 1)
    return jnp.sum(jnp.where(row == lane, a, 0.0), axis=0, keepdims=True)


def in_range(d):
    return (jnp.min(d) > SMALL) & (jnp.max(d) < LARGE)


def factor_kernel(total_rows, odd, kept, received, inverse2, rayleigh, good):
    n = inverse2.shape[0]
    scale = 1.0 / (total_rows**0.5)
    sums1 = jnp.where(odd[0] == 0, kept[...], received[...])
    sums2 = jnp.where(odd[0] == 0, received[...], kept[...])
    gram1, gram2 = [sums[:, :n] * (1.0 / total_rows) for sums in (sums1, sums2)]
    x1, x2 = inverse_factors([gram1, gram2])
    inverse2[...] = x2
    rayleigh[0] = sums1[:, n:].T * scale
    right = nt_dot(sums2[:, n:].T, x1, HIGHEST)
    rayleigh[1] = jnp.dot(x1, right, precision=HIGHEST, preferred_element_type=F32) * scale
    d1 = diagonal(gram1)
    gain = jnp.sum(x1 * x1 * d1) * (1.0 / n)
    fine = in_range(d1) & in_range(diagonal(gram2)) & (gain < GAIN_LIMIT)
    good[0] = (fine & (jnp.max(jnp.abs(x2)) < LARGE)).astype(jnp.int32)


def factor(total_rows, odd, kept, received):
    n = kept.shape[0]
    return pl.pallas_call(
        functools.partial(factor_kernel, total_rows),
        out_shape=(
            jax.ShapeDtypeStruct((n, n), F32),
            jax.ShapeDtypeStruct((2, n, n), F32),
            jax.ShapeDtypeStruct((1,), jnp.int32),
        ),
        in_specs=[smem(), vmem(), vmem()],
        out_specs=(vmem(), vmem(), smem()),
        compiler_params=pltpu.CompilerParams(vmem_limit_bytes=8 << 20),
    )(odd, kept, received)


def from_peer(value, mask):
    devices = lax.axis_size(AXES)
    return lax.ppermute(value, AXES, [(i, i ^ mask) for i in range(devices)])


def sum_halves(kept, given):
    kept = kept + from_peer(given, 1)
    bit, last = 2, lax.axis_size(AXES)
    if last.bit_length() % 2 == 1:
        kept = kept + from_peer(kept, bit)
        bit *= 2
    while bit < last:
        near, far = from_peer(kept, bit), from_peer(kept, 2 * bit)
        kept = (kept + near) + (far + from_peer(kept, 3 * bit))
        bit *= 4
    return kept, from_peer(kept, 1)


def step_by_step(vectors, tiles, counts, tile_col, send_list):
    me = lax.axis_index(AXES)
    outgoing = lax.dynamic_index_in_dim(send_list, me, 0, keepdims=False).reshape(-1)
    devices = lax.axis_size(AXES)
    width, rows_here = vectors.shape
    blocks_here = counts.shape[0]
    tile_size = tiles.shape[1]
    depth = tiles.shape[0] // blocks_here
    total_rows = rows_here * devices
    live = jnp.arange(tiles.shape[0], dtype=jnp.int32) % depth < jnp.repeat(counts, depth)
    live = live.astype(F32)
    current = vectors
    rayleigh = []
    for step in range(ITERS):
        rounded = current.astype(BF16)
        own_blocks = rounded.reshape(width, blocks_here, tile_size).transpose(1, 0, 2)
        parcel = jnp.take(own_blocks, outgoing, axis=0)
        arrived = lax.all_to_all(parcel, AXES, split_axis=0, concat_axis=0, tiled=True)
        picked = jnp.take(arrived, tile_col, axis=0)
        prod = jnp.einsum("jrc,jkc->jkr", tiles, picked, preferred_element_type=F32)
        prod = prod * live[:, None, None]
        image = prod.reshape(blocks_here, depth, width, tile_size).sum(axis=1)
        image = image.transpose(1, 0, 2).reshape(width, rows_here)
        gram_part = jnp.dot(image, image.T, precision=HIGHEST)
        quotient_part = jnp.dot(current, image.T, precision=HIGHEST)
        gram, quotient = lax.psum((gram_part, quotient_part), AXES)
        gram = gram / total_rows
        rayleigh.append(quotient / jnp.sqrt(F32(total_rows)))
        lower = jnp.linalg.cholesky(gram)
        current = lax.linalg.triangular_solve(lower, image, left_side=True, lower=True)
    return current, jnp.stack(rayleigh)


def on_device(vectors, tiles, counts, tile_col, send_list):
    devices = lax.axis_size(AXES)
    total_rows = vectors.shape[1] * devices
    exchange = Exchange(devices, send_list, tiles.shape[1])
    odd = (lax.axis_index(AXES) & 1).reshape(1)
    arrived, cols, odd = exchange(vectors.astype(BF16), exchange.arrival(tile_col), odd)
    image1, rounded = image_of((F32, BF16), counts, cols, arrived, tiles)
    arrived, sums1 = exchange(rounded, first_sums(vectors, image1))
    (image2,) = image_of((F32,), counts, cols, arrived, tiles)
    kept, received = sum_halves(*halves(odd, sums1, image1, image2))
    inverse2, rayleigh, good = factor(total_rows, odd, kept, received)

    def fast():
        return jnp.dot(inverse2, image2, precision=HIGHEST), rayleigh

    def slow():
        return step_by_step(vectors, tiles, counts, tile_col, send_list)

    return lax.cond(good[0] > 0, fast, slow)


def solution(mesh):
    return jax.shard_map(
        on_device,
        mesh=mesh,
        in_specs=(
            P(None, AXES),
            P(AXES, None, None),
            P(AXES),
            P(AXES),
            P(),
        ),
        out_specs=(P(None, AXES), P()),
        check_vma=False,
    )
```

```python
import functools

import jax
import jax.numpy as jnp
from jax import lax
from jax.experimental import pallas as pl
from jax.experimental.pallas import tpu as pltpu
from jax.sharding import PartitionSpec as P

ITERS = 2
AXES = ("gx", "gy")
F32 = jnp.float32
BF16 = jnp.bfloat16
HIGHEST = lax.Precision.HIGHEST

GAIN_LIMIT = 1.5
SMALL, LARGE = 1e-25, 1e25
STEP = 4


def vmem():
    return pl.BlockSpec(memory_space=pltpu.VMEM)


def smem():
    return pl.BlockSpec(memory_space=pltpu.SMEM)


def nt_dot(a, b, precision=None):
    return lax.dot_general(
        a, b, (((1,), (1,)), ((), ())), precision=precision, preferred_element_type=F32
    )


def pack_kernel(outgoing, own, other, parcel):
    peers, rows, tile = parcel.shape
    width = own.shape[0]
    slots = rows // width // 2

    def one(p, carry):
        for i, source in enumerate((own, other)):
            for slot in range(slots):
                block = outgoing[(i * peers + p) * slots + slot]
                at = (i * slots + slot) * width
                parcel[p, at : at + width, :] = source[:, pl.ds(pl.multiple_of(block * tile, tile), tile)]
        return carry

    lax.fori_loop(0, peers, one, 0, unroll=8)


def pack(outgoing, own, other, peers, tile):
    width = own.shape[0]
    rows = outgoing.shape[0] // peers * width
    return pl.pallas_call(
        pack_kernel,
        out_shape=jax.ShapeDtypeStruct((peers, rows, tile), BF16),
        in_specs=[smem(), vmem(), vmem()],
        out_specs=vmem(),
        compiler_params=pltpu.CompilerParams(vmem_limit_bytes=4 << 20),
        cost_estimate=pl.CostEstimate(
            flops=5_000_000_000, bytes_accessed=32 << 20, transcendentals=0
        ),
    )(outgoing, own, other)


class Exchange:
    def __init__(self, devices, send_list, tile):
        assert devices >= 4 and devices & (devices - 1) == 0
        self.peers = half = devices // 2
        self.swap = [(i, i ^ half) for i in range(devices)]
        self.groups = [list(range(half)), list(range(half, devices))]
        self.tile = tile
        self.slots = send_list.shape[2]
        me = lax.axis_index(AXES)
        self.side = (me >= half).astype(jnp.int32)
        lists = [
            lax.dynamic_slice(send_list, (source, self.side * half, 0), (1, half, self.slots))
            for source in (me, me ^ half)
        ]
        self.outgoing = jnp.concatenate(lists).reshape(-1)

    def arrival(self, tile_col):
        sender, slot = tile_col // self.slots, tile_col % self.slots
        far = (sender >= self.peers).astype(jnp.int32) ^ self.side
        return (2 * (sender % self.peers) + far) * self.slots + slot

    def __call__(self, rounded, *ahead):
        other = lax.ppermute(rounded, AXES, self.swap)
        parcel = pack(self.outgoing, rounded, other, self.peers, self.tile)
        parcel, *ahead = lax.optimization_barrier((parcel, *ahead))
        arrived = lax.all_to_all(
            parcel, AXES, split_axis=0, concat_axis=0, axis_index_groups=self.groups, tiled=True
        )
        return (arrived.reshape(-1, rounded.shape[0], self.tile), *ahead)


def image_kernel(blocks, plan, arrived, tiles, image, *rounded):
    depth = tiles.shape[0] // blocks
    tile = tiles.shape[1]
    width = arrived.shape[1]
    mxus = (0, 1)

    def push(b, t, register, mxu):
        pltpu.matmul_push_rhs(
            tiles[b * depth + t], staging_register=register, mxu_index=mxu, transpose=True
        )

    def block(b, t):
        found = arrived[plan[blocks + b * depth + t]]
        return jnp.where(t < plan[b], found, jnp.zeros_like(found))

    def run(*refs):
        sums = (refs[0:2], refs[2:4])
        spare = refs[4:6]
        for ref in refs:
            pltpu.matmul_pop(ref)

        def flush(b):
            first, second = sums[b % 2]
            value = pltpu.matmul_pop(first) + pltpu.matmul_pop(second)
            for ref in (image, *rounded):
                ref[:, b * tile : (b + 1) * tile] = value.astype(ref.dtype)

        for mxu in mxus:
            push(0, mxu, 0, mxu)
        for b in range(blocks):
            steps = (plan[b] + STEP - 1) // STEP

            def products(t, push_next):
                for mxu in mxus:
                    push(b, t + 2 + mxu, 1, mxu)
                for mxu in mxus:
                    pltpu.matmul_acc_lhs(sums[b % 2][mxu], block(b, t + mxu), load_staged_rhs=0)
                for mxu in mxus:
                    push_next(mxu)
                for mxu in mxus:
                    pltpu.matmul_acc_lhs(sums[b % 2][mxu], block(b, t + 2 + mxu), load_staged_rhs=1)

            def step(q, carry):
                products(q * STEP, lambda mxu: push(b, (q + 1) * STEP + mxu, 0, mxu))
                return carry

            lax.fori_loop(0, steps - 1, step, 0)
            products((steps - 1) * STEP, lambda mxu: push(min(b + 1, blocks - 1), mxu, 0, mxu))
            if b:
                flush(b - 1)
        for mxu in mxus:
            pltpu.matmul_acc_lhs(spare[mxu], jnp.zeros((16, tile), BF16), load_staged_rhs=0)
        flush(blocks - 1)
        for ref in spare:
            pltpu.matmul_pop(ref)

    pl.run_scoped(
        run,
        *[pltpu.ACC(mxu)((width, tile), F32) for mxu in mxus + mxus],
        *[pltpu.ACC(mxu)((16, tile), F32) for mxu in mxus],
    )


def image_of(kinds, plan, arrived, tiles):
    width, tile = arrived.shape[1:]
    blocks = plan.shape[0] - tiles.shape[0]
    assert tile == 256 and width % 16 == 0 and width <= 256
    assert tiles.shape[0] % (blocks * STEP) == 0
    grant = (4 if 16 * arrived.size <= tiles.size else 24) << 20
    return pl.pallas_call(
        functools.partial(image_kernel, blocks),
        out_shape=[jax.ShapeDtypeStruct((width, blocks * tile), kind) for kind in kinds],
        in_specs=[smem(), vmem(), vmem()],
        out_specs=[vmem()] * len(kinds),
        compiler_params=pltpu.CompilerParams(vmem_limit_bytes=grant),
        cost_estimate=pl.CostEstimate(
            flops=width * tiles.size, bytes_accessed=tiles.size, transcendentals=0
        ),
    )(plan, arrived, tiles)


def first_sums_kernel(vectors, image, sums):
    sums[...] = nt_dot(image[...], jnp.concatenate([image[...], vectors[...]], axis=0), HIGHEST)


def first_sums(vectors, image):
    n = vectors.shape[0]
    return pl.pallas_call(
        first_sums_kernel,
        out_shape=jax.ShapeDtypeStruct((n, 2 * n), F32),
        in_specs=[vmem()] * 2,
        out_specs=vmem(),
        compiler_params=pltpu.CompilerParams(vmem_limit_bytes=4 << 20),
    )(vectors, image)


def halves_kernel(odd, sums1, image1, image2, kept, given):
    sums2 = nt_dot(image2[...], jnp.concatenate([image2[...], image1[...]], axis=0), HIGHEST)
    for when, mine, other in ((0, sums1, None), (1, None, sums1)):

        @pl.when(odd[0] == when)
        def _():
            kept[...] = sums2 if mine is None else mine[...]
            given[...] = sums2 if other is None else other[...]


def halves(odd, sums1, image1, image2):
    shape = jax.ShapeDtypeStruct(sums1.shape, F32)
    return pl.pallas_call(
        halves_kernel,
        out_shape=(shape, shape),
        in_specs=[smem()] + [vmem()] * 3,
        out_specs=(vmem(), vmem()),
        compiler_params=pltpu.CompilerParams(vmem_limit_bytes=4 << 20),
    )(odd, sums1, image1, image2)


def inverse_factors(grams):
    n = grams[0].shape[0]
    wide = 2 * n
    group = 8
    pieces = n // group
    sub = lax.broadcasted_iota(jnp.int32, (group, wide), 0)
    lane = lax.broadcasted_iota(jnp.int32, (group, wide), 1)

    def spread(row):
        return jnp.broadcast_to(row, (group, wide))

    held = []
    for a in grams:
        rows = []
        for r in range(pieces):
            eye = (lane == sub + (n + group * r)).astype(F32)[:, n:]
            rows.append(jnp.concatenate([a[group * r : group * (r + 1), :], eye], axis=1))
        held.append(rows)
    pivots = [[] for _ in grams]
    for k in range(pieces):
        columns = [
            [[spread(m[r][:, j : j + 1]) for r in range(k, pieces)] for j in range(group * k, group * (k + 1))]
            for m in held
        ]
        found = [jnp.ones((group, wide), F32) for _ in grams]
        for j in range(group):
            for p, m in enumerate(held):
                column = columns[p]
                pivot = spread(column[j][0][j : j + 1, :])
                found[p] = jnp.where(sub == j, pivot, found[p])
                scale = 1.0 / pivot
                row = spread(m[k][j : j + 1, :])
                later = [spread(column[i][0][j : j + 1, :]) for i in range(j + 1, group)]
                for r in range(k, pieces):
                    factor = column[j][r - k] * scale
                    if r == k:
                        factor = jnp.where(sub > j, factor, 0.0)
                    m[r] = m[r] - factor * row
                    for i in range(j + 1, group):
                        column[i][r - k] = column[i][r - k] - factor * later[i - j - 1]
        for p in range(len(grams)):
            pivots[p].append(found[p])
    return [
        jnp.concatenate(
            [(held[p][r] / jnp.sqrt(pivots[p][r]))[:, n:] for r in range(pieces)], axis=0
        )
        for p in range(len(grams))
    ]


def diagonal(a):
    n = a.shape[0]
    row = lax.broadcasted_iota(jnp.int32, (n, n), 0)
    lane = lax.broadcasted_iota(jnp.int32, (n, n), 1)
    return jnp.sum(jnp.where(row == lane, a, 0.0), axis=0, keepdims=True)


def in_range(d):
    return (jnp.min(d) > SMALL) & (jnp.max(d) < LARGE)


def factor_kernel(total_rows, odd, kept, received, inverse2, rayleigh, good):
    n = inverse2.shape[0]
    scale = 1.0 / (total_rows**0.5)
    sums1 = jnp.where(odd[0] == 0, kept[...], received[...])
    sums2 = jnp.where(odd[0] == 0, received[...], kept[...])
    gram1, gram2 = [sums[:, :n] * (1.0 / total_rows) for sums in (sums1, sums2)]
    x1, x2 = inverse_factors([gram1, gram2])
    inverse2[...] = x2
    rayleigh[0] = sums1[:, n:].T * scale
    right = nt_dot(sums2[:, n:].T, x1, HIGHEST)
    rayleigh[1] = jnp.dot(x1, right, precision=HIGHEST, preferred_element_type=F32) * scale
    d1 = diagonal(gram1)
    gain = jnp.sum(x1 * x1 * d1) * (1.0 / n)
    fine = in_range(d1) & in_range(diagonal(gram2)) & (gain < GAIN_LIMIT)
    good[0] = (fine & (jnp.max(jnp.abs(x2)) < LARGE)).astype(jnp.int32)


def factor(total_rows, odd, kept, received):
    n = kept.shape[0]
    return pl.pallas_call(
        functools.partial(factor_kernel, total_rows),
        out_shape=(
            jax.ShapeDtypeStruct((n, n), F32),
            jax.ShapeDtypeStruct((2, n, n), F32),
            pltpu.MemorySpace.SMEM((1,), jnp.int32),
        ),
        in_specs=[smem(), vmem(), vmem()],
        out_specs=(vmem(), vmem(), smem()),
        compiler_params=pltpu.CompilerParams(vmem_limit_bytes=8 << 20),
    )(odd, kept, received)


def from_peer(value, mask):
    devices = lax.axis_size(AXES)
    return lax.ppermute(value, AXES, [(i, i ^ mask) for i in range(devices)])


def sum_halves(kept, given):
    kept = kept + from_peer(given, 1)
    bit, last = 2, lax.axis_size(AXES)
    if last.bit_length() % 2 == 1:
        kept = kept + from_peer(kept, bit)
        bit *= 2
    while bit < last:
        near, far = from_peer(kept, bit), from_peer(kept, 2 * bit)
        kept = (kept + near) + (far + from_peer(kept, 3 * bit))
        bit *= 4
    return kept, from_peer(kept, 1)


def step_by_step(vectors, tiles, counts, tile_col, send_list):
    me = lax.axis_index(AXES)
    outgoing = lax.dynamic_index_in_dim(send_list, me, 0, keepdims=False).reshape(-1)
    devices = lax.axis_size(AXES)
    width, rows_here = vectors.shape
    blocks_here = counts.shape[0]
    tile_size = tiles.shape[1]
    depth = tiles.shape[0] // blocks_here
    total_rows = rows_here * devices
    live = jnp.arange(tiles.shape[0], dtype=jnp.int32) % depth < jnp.repeat(counts, depth)
    live = live.astype(F32)
    current = vectors
    rayleigh = []
    for step in range(ITERS):
        rounded = current.astype(BF16)
        own_blocks = rounded.reshape(width, blocks_here, tile_size).transpose(1, 0, 2)
        parcel = jnp.take(own_blocks, outgoing, axis=0)
        arrived = lax.all_to_all(parcel, AXES, split_axis=0, concat_axis=0, tiled=True)
        picked = jnp.take(arrived, tile_col, axis=0)
        prod = jnp.einsum("jrc,jkc->jkr", tiles, picked, preferred_element_type=F32)
        prod = prod * live[:, None, None]
        image = prod.reshape(blocks_here, depth, width, tile_size).sum(axis=1)
        image = image.transpose(1, 0, 2).reshape(width, rows_here)
        gram_part = jnp.dot(image, image.T, precision=HIGHEST)
        quotient_part = jnp.dot(current, image.T, precision=HIGHEST)
        gram, quotient = lax.psum((gram_part, quotient_part), AXES)
        gram = gram / total_rows
        rayleigh.append(quotient / jnp.sqrt(F32(total_rows)))
        lower = jnp.linalg.cholesky(gram)
        current = lax.linalg.triangular_solve(lower, image, left_side=True, lower=True)
    return current, jnp.stack(rayleigh)


def on_device(vectors, tiles, counts, tile_col, send_list):
    devices = lax.axis_size(AXES)
    total_rows = vectors.shape[1] * devices
    exchange = Exchange(devices, send_list, tiles.shape[1])
    odd = (lax.axis_index(AXES) & 1).reshape(1)
    plan = jnp.concatenate([counts, exchange.arrival(tile_col)])
    arrived, plan, odd = exchange(vectors.astype(BF16), plan, odd)
    image1, rounded = image_of((F32, BF16), plan, arrived, tiles)
    arrived, sums1 = exchange(rounded, first_sums(vectors, image1))
    (image2,) = image_of((F32,), plan, arrived, tiles)
    kept, received = sum_halves(*halves(odd, sums1, image1, image2))
    inverse2, rayleigh, good = factor(total_rows, odd, kept, received)

    def fast():
        return jnp.dot(inverse2, image2, precision=HIGHEST), rayleigh

    def slow():
        return step_by_step(vectors, tiles, counts, tile_col, send_list)

    return lax.cond(good[0] > 0, fast, slow)


def solution(mesh):
    return jax.shard_map(
        on_device,
        mesh=mesh,
        in_specs=(
            P(None, AXES),
            P(AXES, None, None),
            P(AXES),
            P(AXES),
            P(),
        ),
        out_specs=(P(None, AXES), P()),
        check_vma=False,
    )
```

```python
import functools

import jax
import jax.numpy as jnp
from jax import lax
from jax.experimental import pallas as pl
from jax.experimental.pallas import tpu as pltpu
from jax.sharding import PartitionSpec as P

ITERS = 2
AXES = ("gx", "gy")
F32 = jnp.float32
BF16 = jnp.bfloat16
HIGHEST = lax.Precision.HIGHEST

GAIN_LIMIT = 1.5
SMALL, LARGE = 1e-25, 1e25
STEP = 4


def vmem():
    return pl.BlockSpec(memory_space=pltpu.VMEM)


def smem():
    return pl.BlockSpec(memory_space=pltpu.SMEM)


def nt_dot(a, b, precision=None):
    return lax.dot_general(
        a, b, (((1,), (1,)), ((), ())), precision=precision, preferred_element_type=F32
    )


def pack_kernel(outgoing, own, other, parcel):
    peers, rows, tile = parcel.shape
    width = own.shape[0]
    slots = rows // width // 2

    def one(p, carry):
        for i, source in enumerate((own, other)):
            for slot in range(slots):
                block = outgoing[(i * peers + p) * slots + slot]
                at = (i * slots + slot) * width
                parcel[p, at : at + width, :] = source[:, pl.ds(pl.multiple_of(block * tile, tile), tile)]
        return carry

    lax.fori_loop(0, peers, one, 0, unroll=8)


def pack(outgoing, own, other, peers, tile):
    width = own.shape[0]
    rows = outgoing.shape[0] // peers * width
    return pl.pallas_call(
        pack_kernel,
        out_shape=jax.ShapeDtypeStruct((peers, rows, tile), BF16),
        in_specs=[smem(), vmem(), vmem()],
        out_specs=vmem(),
        compiler_params=pltpu.CompilerParams(vmem_limit_bytes=4 << 20),
        cost_estimate=pl.CostEstimate(
            flops=5_000_000_000, bytes_accessed=32 << 20, transcendentals=0
        ),
    )(outgoing, own, other)


class Exchange:
    def __init__(self, devices, send_list, tile):
        assert devices >= 4 and devices & (devices - 1) == 0
        self.peers = half = devices // 2
        self.swap = [(i, i ^ half) for i in range(devices)]
        self.groups = [list(range(half)), list(range(half, devices))]
        self.tile = tile
        self.slots = send_list.shape[2]
        me = lax.axis_index(AXES)
        self.side = (me >= half).astype(jnp.int32)
        lists = [
            lax.dynamic_slice(send_list, (source, self.side * half, 0), (1, half, self.slots))
            for source in (me, me ^ half)
        ]
        self.outgoing = jnp.concatenate(lists).reshape(-1)

    def arrival(self, tile_col):
        sender, slot = tile_col // self.slots, tile_col % self.slots
        far = (sender >= self.peers).astype(jnp.int32) ^ self.side
        return (2 * (sender % self.peers) + far) * self.slots + slot

    def __call__(self, rounded, *ahead):
        other = lax.ppermute(rounded, AXES, self.swap)
        parcel = pack(self.outgoing, rounded, other, self.peers, self.tile)
        parcel, *ahead = lax.optimization_barrier((parcel, *ahead))
        arrived = lax.all_to_all(
            parcel, AXES, split_axis=0, concat_axis=0, axis_index_groups=self.groups, tiled=True
        )
        return (arrived.reshape(-1, rounded.shape[0], self.tile), *ahead)


def image_kernel(blocks, plan, arrived, tiles, image, *rounded):
    depth = tiles.shape[0] // blocks
    tile = tiles.shape[1]
    width = arrived.shape[1]
    mxus = (0, 1)

    def push(b, t, register, mxu):
        pltpu.matmul_push_rhs(
            tiles[b * depth + t], staging_register=register, mxu_index=mxu, transpose=True
        )

    def block(b, t):
        found = arrived[plan[blocks + b * depth + t]]
        return jnp.where(t < plan[b], found, jnp.zeros_like(found))

    def run(*refs):
        sums = (refs[0:2], refs[2:4])
        spare = refs[4:6]
        for ref in refs:
            pltpu.matmul_pop(ref)

        def flush(b):
            first, second = sums[b % 2]
            value = pltpu.matmul_pop(first) + pltpu.matmul_pop(second)
            for ref in (image, *rounded):
                ref[:, b * tile : (b + 1) * tile] = value.astype(ref.dtype)

        for mxu in mxus:
            push(0, mxu, 0, mxu)
        for b in range(blocks):
            steps = (plan[b] + STEP - 1) // STEP

            def products(t, push_next):
                for mxu in mxus:
                    push(b, t + 2 + mxu, 1, mxu)
                for mxu in mxus:
                    pltpu.matmul_acc_lhs(sums[b % 2][mxu], block(b, t + mxu), load_staged_rhs=0)
                for mxu in mxus:
                    push_next(mxu)
                for mxu in mxus:
                    pltpu.matmul_acc_lhs(sums[b % 2][mxu], block(b, t + 2 + mxu), load_staged_rhs=1)

            def step(q, carry):
                products(q * STEP, lambda mxu: push(b, (q + 1) * STEP + mxu, 0, mxu))
                return carry

            lax.fori_loop(0, steps - 1, step, 0)
            products((steps - 1) * STEP, lambda mxu: push(min(b + 1, blocks - 1), mxu, 0, mxu))
            if b:
                flush(b - 1)
        for mxu in mxus:
            pltpu.matmul_acc_lhs(spare[mxu], jnp.zeros((16, tile), BF16), load_staged_rhs=0)
        flush(blocks - 1)
        for ref in spare:
            pltpu.matmul_pop(ref)

    pl.run_scoped(
        run,
        *[pltpu.ACC(mxu)((width, tile), F32) for mxu in mxus + mxus],
        *[pltpu.ACC(mxu)((16, tile), F32) for mxu in mxus],
    )


def image_of(kinds, plan, arrived, tiles):
    width, tile = arrived.shape[1:]
    blocks = plan.shape[0] - tiles.shape[0]
    assert tile == 256 and width % 16 == 0 and width <= 256
    assert tiles.shape[0] % (blocks * STEP) == 0
    grant = (4 if 16 * arrived.size <= tiles.size else 24) << 20
    return pl.pallas_call(
        functools.partial(image_kernel, blocks),
        out_shape=[jax.ShapeDtypeStruct((width, blocks * tile), kind) for kind in kinds],
        in_specs=[smem(), vmem(), vmem()],
        out_specs=[vmem()] * len(kinds),
        compiler_params=pltpu.CompilerParams(vmem_limit_bytes=grant),
        cost_estimate=pl.CostEstimate(
            flops=width * tiles.size, bytes_accessed=tiles.size, transcendentals=0
        ),
    )(plan, arrived, tiles)


def first_sums_kernel(vectors, image, sums):
    sums[...] = nt_dot(image[...], jnp.concatenate([image[...], vectors[...]], axis=0), HIGHEST)


def first_sums(vectors, image):
    n = vectors.shape[0]
    return pl.pallas_call(
        first_sums_kernel,
        out_shape=jax.ShapeDtypeStruct((n, 2 * n), F32),
        in_specs=[vmem()] * 2,
        out_specs=vmem(),
        compiler_params=pltpu.CompilerParams(vmem_limit_bytes=4 << 20),
    )(vectors, image)


def halves_kernel(odd, sums1, image1, image2, kept, given):
    sums2 = nt_dot(image2[...], jnp.concatenate([image2[...], image1[...]], axis=0), HIGHEST)
    for when, mine, other in ((0, sums1, None), (1, None, sums1)):

        @pl.when(odd[0] == when)
        def _():
            kept[...] = sums2 if mine is None else mine[...]
            given[...] = sums2 if other is None else other[...]


def halves(odd, sums1, image1, image2):
    shape = jax.ShapeDtypeStruct(sums1.shape, F32)
    return pl.pallas_call(
        halves_kernel,
        out_shape=(shape, shape),
        in_specs=[smem()] + [vmem()] * 3,
        out_specs=(vmem(), vmem()),
        compiler_params=pltpu.CompilerParams(vmem_limit_bytes=4 << 20),
    )(odd, sums1, image1, image2)


def inverse_factors(grams):
    n = grams[0].shape[0]
    wide = 2 * n
    group = 8
    pieces = n // group
    sub = lax.broadcasted_iota(jnp.int32, (group, wide), 0)
    lane = lax.broadcasted_iota(jnp.int32, (group, wide), 1)

    def spread(row):
        return jnp.broadcast_to(row, (group, wide))

    held = []
    for a in grams:
        rows = []
        for r in range(pieces):
            eye = (lane == sub + (n + group * r)).astype(F32)[:, n:]
            rows.append(jnp.concatenate([a[group * r : group * (r + 1), :], eye], axis=1))
        held.append(rows)
    pivots = [[] for _ in grams]
    for k in range(pieces):
        columns = [
            [[spread(m[r][:, j : j + 1]) for r in range(k, pieces)] for j in range(group * k, group * (k + 1))]
            for m in held
        ]
        found = [jnp.ones((group, wide), F32) for _ in grams]
        for j in range(group):
            for p, m in enumerate(held):
                column = columns[p]
                pivot = spread(column[j][0][j : j + 1, :])
                found[p] = jnp.where(sub == j, pivot, found[p])
                scale = 1.0 / pivot
                row = spread(m[k][j : j + 1, :])
                later = [spread(column[i][0][j : j + 1, :]) for i in range(j + 1, group)]
                for r in range(k, pieces):
                    factor = column[j][r - k] * scale
                    if r == k:
                        factor = jnp.where(sub > j, factor, 0.0)
                    m[r] = m[r] - factor * row
                    for i in range(j + 1, group):
                        column[i][r - k] = column[i][r - k] - factor * later[i - j - 1]
        for p in range(len(grams)):
            pivots[p].append(found[p])
    return [
        jnp.concatenate(
            [(held[p][r] / jnp.sqrt(pivots[p][r]))[:, n:] for r in range(pieces)], axis=0
        )
        for p in range(len(grams))
    ]


def diagonal(a):
    n = a.shape[0]
    row = lax.broadcasted_iota(jnp.int32, (n, n), 0)
    lane = lax.broadcasted_iota(jnp.int32, (n, n), 1)
    return jnp.sum(jnp.where(row == lane, a, 0.0), axis=0, keepdims=True)


def in_range(d):
    return (jnp.min(d) > SMALL) & (jnp.max(d) < LARGE)


def factor_kernel(total_rows, odd, kept, received, inverse2, rayleigh, good):
    n = inverse2.shape[0]
    scale = 1.0 / (total_rows**0.5)
    sums1 = jnp.where(odd[0] == 0, kept[...], received[...])
    sums2 = jnp.where(odd[0] == 0, received[...], kept[...])
    gram1, gram2 = [sums[:, :n] * (1.0 / total_rows) for sums in (sums1, sums2)]
    x1, x2 = inverse_factors([gram1, gram2])
    inverse2[...] = x2
    rayleigh[0] = sums1[:, n:].T * scale
    right = nt_dot(sums2[:, n:].T, x1, HIGHEST)
    rayleigh[1] = jnp.dot(x1, right, precision=HIGHEST, preferred_element_type=F32) * scale
    fine = True
    for gram, x in ((gram1, x1), (gram2, x2)):
        d = diagonal(gram)
        fine = fine & in_range(d) & (jnp.sum(x * x * d) < GAIN_LIMIT * n)
    good[0] = fine.astype(jnp.int32)


def factor(total_rows, odd, kept, received):
    n = kept.shape[0]
    return pl.pallas_call(
        functools.partial(factor_kernel, total_rows),
        out_shape=(
            jax.ShapeDtypeStruct((n, n), F32),
            jax.ShapeDtypeStruct((2, n, n), F32),
            pltpu.MemorySpace.SMEM((1,), jnp.int32),
        ),
        in_specs=[smem(), vmem(), vmem()],
        out_specs=(vmem(), vmem(), smem()),
        compiler_params=pltpu.CompilerParams(vmem_limit_bytes=8 << 20),
    )(odd, kept, received)


def from_peer(value, mask):
    devices = lax.axis_size(AXES)
    return lax.ppermute(value, AXES, [(i, i ^ mask) for i in range(devices)])


def sum_halves(kept, given):
    kept = kept + from_peer(given, 1)
    bit, last = 2, lax.axis_size(AXES)
    if last.bit_length() % 2 == 1:
        kept = kept + from_peer(kept, bit)
        bit *= 2
    while bit < last:
        near, far = from_peer(kept, bit), from_peer(kept, 2 * bit)
        kept = (kept + near) + (far + from_peer(kept, 3 * bit))
        bit *= 4
    return kept, from_peer(kept, 1)


def step_by_step(vectors, tiles, counts, tile_col, send_list):
    me = lax.axis_index(AXES)
    outgoing = lax.dynamic_index_in_dim(send_list, me, 0, keepdims=False).reshape(-1)
    devices = lax.axis_size(AXES)
    width, rows_here = vectors.shape
    blocks_here = counts.shape[0]
    tile_size = tiles.shape[1]
    depth = tiles.shape[0] // blocks_here
    total_rows = rows_here * devices
    live = jnp.arange(tiles.shape[0], dtype=jnp.int32) % depth < jnp.repeat(counts, depth)
    live = live.astype(F32)
    current = vectors
    rayleigh = []
    for step in range(ITERS):
        rounded = current.astype(BF16)
        own_blocks = rounded.reshape(width, blocks_here, tile_size).transpose(1, 0, 2)
        parcel = jnp.take(own_blocks, outgoing, axis=0)
        arrived = lax.all_to_all(parcel, AXES, split_axis=0, concat_axis=0, tiled=True)
        picked = jnp.take(arrived, tile_col, axis=0)
        prod = jnp.einsum("jrc,jkc->jkr", tiles, picked, preferred_element_type=F32)
        prod = prod * live[:, None, None]
        image = prod.reshape(blocks_here, depth, width, tile_size).sum(axis=1)
        image = image.transpose(1, 0, 2).reshape(width, rows_here)
        gram_part = jnp.dot(image, image.T, precision=HIGHEST)
        quotient_part = jnp.dot(current, image.T, precision=HIGHEST)
        gram, quotient = lax.psum((gram_part, quotient_part), AXES)
        gram = gram / total_rows
        rayleigh.append(quotient / jnp.sqrt(F32(total_rows)))
        lower = jnp.linalg.cholesky(gram)
        current = lax.linalg.triangular_solve(lower, image, left_side=True, lower=True)
    return current, jnp.stack(rayleigh)


def on_device(vectors, tiles, counts, tile_col, send_list):
    devices = lax.axis_size(AXES)
    total_rows = vectors.shape[1] * devices
    exchange = Exchange(devices, send_list, tiles.shape[1])
    odd = (lax.axis_index(AXES) & 1).reshape(1)
    plan = jnp.concatenate([counts, exchange.arrival(tile_col)])
    arrived, plan, odd = exchange(vectors.astype(BF16), plan, odd)
    image1, rounded = image_of((F32, BF16), plan, arrived, tiles)
    arrived, sums1 = exchange(rounded, first_sums(vectors, image1))
    (image2,) = image_of((F32,), plan, arrived, tiles)
    kept, received = sum_halves(*halves(odd, sums1, image1, image2))
    inverse2, rayleigh, good = factor(total_rows, odd, kept, received)

    def fast():
        return jnp.dot(inverse2, image2, precision=HIGHEST), rayleigh

    def slow():
        return step_by_step(vectors, tiles, counts, tile_col, send_list)

    return lax.cond(good[0] > 0, fast, slow)


def solution(mesh):
    return jax.shard_map(
        on_device,
        mesh=mesh,
        in_specs=(
            P(None, AXES),
            P(AXES, None, None),
            P(AXES),
            P(AXES),
            P(),
        ),
        out_specs=(P(None, AXES), P()),
        check_vma=False,
    )
```

```python
import functools

import jax
import jax.numpy as jnp
from jax import lax
from jax.experimental import pallas as pl
from jax.experimental.pallas import tpu as pltpu
from jax.sharding import PartitionSpec as P

ITERS = 2
AXES = ("gx", "gy")
F32 = jnp.float32
BF16 = jnp.bfloat16
HIGHEST = lax.Precision.HIGHEST

GAIN_LIMIT = 1.5
SMALL, LARGE = 1e-25, 1e25
STEP = 4


def vmem():
    return pl.BlockSpec(memory_space=pltpu.VMEM)


def smem():
    return pl.BlockSpec(memory_space=pltpu.SMEM)


def nt_dot(a, b, precision=None):
    return lax.dot_general(
        a, b, (((1,), (1,)), ((), ())), precision=precision, preferred_element_type=F32
    )


def pack_kernel(outgoing, own, other, parcel):
    peers, rows, tile = parcel.shape
    width = own.shape[0]
    slots = rows // width // 2

    def one(p, carry):
        for i, source in enumerate((own, other)):
            for slot in range(slots):
                block = outgoing[(i * peers + p) * slots + slot]
                at = (i * slots + slot) * width
                parcel[p, at : at + width, :] = source[:, pl.ds(pl.multiple_of(block * tile, tile), tile)]
        return carry

    lax.fori_loop(0, peers, one, 0, unroll=16)


def pack(outgoing, own, other, peers, tile):
    width = own.shape[0]
    rows = outgoing.shape[0] // peers * width
    return pl.pallas_call(
        pack_kernel,
        out_shape=jax.ShapeDtypeStruct((peers, rows, tile), BF16),
        in_specs=[smem(), vmem(), vmem()],
        out_specs=vmem(),
        compiler_params=pltpu.CompilerParams(vmem_limit_bytes=4 << 20),
        cost_estimate=pl.CostEstimate(
            flops=5_000_000_000, bytes_accessed=32 << 20, transcendentals=0
        ),
    )(outgoing, own, other)


class Exchange:
    def __init__(self, devices, send_list, tile):
        assert devices >= 4 and devices & (devices - 1) == 0
        self.peers = half = devices // 2
        self.swap = [(i, i ^ half) for i in range(devices)]
        self.groups = [list(range(half)), list(range(half, devices))]
        self.tile = tile
        self.slots = send_list.shape[2]
        me = lax.axis_index(AXES)
        self.side = (me >= half).astype(jnp.int32)
        lists = [
            lax.dynamic_slice(send_list, (source, self.side * half, 0), (1, half, self.slots))
            for source in (me, me ^ half)
        ]
        self.outgoing = jnp.concatenate(lists).reshape(-1)

    def arrival(self, tile_col):
        sender, slot = tile_col // self.slots, tile_col % self.slots
        far = (sender >= self.peers).astype(jnp.int32) ^ self.side
        return (2 * (sender % self.peers) + far) * self.slots + slot

    def __call__(self, rounded, *ahead):
        other = lax.ppermute(rounded, AXES, self.swap)
        parcel = pack(self.outgoing, rounded, other, self.peers, self.tile)
        parcel, *ahead = lax.optimization_barrier((parcel, *ahead))
        arrived = lax.all_to_all(
            parcel, AXES, split_axis=0, concat_axis=0, axis_index_groups=self.groups, tiled=True
        )
        return (arrived.reshape(-1, rounded.shape[0], self.tile), *ahead)


def image_kernel(blocks, plan, arrived, tiles, image, *rounded):
    depth = tiles.shape[0] // blocks
    tile = tiles.shape[1]
    width = arrived.shape[1]
    mxus = (0, 1)

    def push(b, t, register, mxu):
        pltpu.matmul_push_rhs(
            tiles[b * depth + t], staging_register=register, mxu_index=mxu, transpose=True
        )

    def block(b, t):
        found = arrived[plan[blocks + b * depth + t]]
        return jnp.where(t < plan[b], found, jnp.zeros_like(found))

    def run(*refs):
        sums = (refs[0:2], refs[2:4])
        spare = refs[4:6]
        for ref in refs:
            pltpu.matmul_pop(ref)

        def flush(b):
            first, second = sums[b % 2]
            value = pltpu.matmul_pop(first) + pltpu.matmul_pop(second)
            for ref in (image, *rounded):
                ref[:, b * tile : (b + 1) * tile] = value.astype(ref.dtype)

        for mxu in mxus:
            push(0, mxu, 0, mxu)
        for b in range(blocks):
            steps = (plan[b] + STEP - 1) // STEP

            def products(t, push_next):
                for mxu in mxus:
                    push(b, t + 2 + mxu, 1, mxu)
                for mxu in mxus:
                    pltpu.matmul_acc_lhs(sums[b % 2][mxu], block(b, t + mxu), load_staged_rhs=0)
                for mxu in mxus:
                    push_next(mxu)
                for mxu in mxus:
                    pltpu.matmul_acc_lhs(sums[b % 2][mxu], block(b, t + 2 + mxu), load_staged_rhs=1)

            def step(q, carry):
                products(q * STEP, lambda mxu: push(b, (q + 1) * STEP + mxu, 0, mxu))
                return carry

            lax.fori_loop(0, steps - 1, step, 0)
            products((steps - 1) * STEP, lambda mxu: push(min(b + 1, blocks - 1), mxu, 0, mxu))
            if b:
                flush(b - 1)
        for mxu in mxus:
            pltpu.matmul_acc_lhs(spare[mxu], jnp.zeros((16, tile), BF16), load_staged_rhs=0)
        flush(blocks - 1)
        for ref in spare:
            pltpu.matmul_pop(ref)

    pl.run_scoped(
        run,
        *[pltpu.ACC(mxu)((width, tile), F32) for mxu in mxus + mxus],
        *[pltpu.ACC(mxu)((16, tile), F32) for mxu in mxus],
    )


def image_of(kinds, plan, arrived, tiles):
    width, tile = arrived.shape[1:]
    blocks = plan.shape[0] - tiles.shape[0]
    assert tile == 256 and width % 16 == 0 and width <= 256
    assert tiles.shape[0] % (blocks * STEP) == 0
    grant = (4 if 16 * arrived.size <= tiles.size else 24) << 20
    return pl.pallas_call(
        functools.partial(image_kernel, blocks),
        out_shape=[jax.ShapeDtypeStruct((width, blocks * tile), kind) for kind in kinds],
        in_specs=[smem(), vmem(), vmem()],
        out_specs=[vmem()] * len(kinds),
        compiler_params=pltpu.CompilerParams(vmem_limit_bytes=grant),
        cost_estimate=pl.CostEstimate(
            flops=width * tiles.size, bytes_accessed=tiles.size, transcendentals=0
        ),
    )(plan, arrived, tiles)


def first_sums_kernel(vectors, image, sums):
    sums[...] = nt_dot(image[...], jnp.concatenate([image[...], vectors[...]], axis=0), HIGHEST)


def first_sums(vectors, image):
    n = vectors.shape[0]
    return pl.pallas_call(
        first_sums_kernel,
        out_shape=jax.ShapeDtypeStruct((n, 2 * n), F32),
        in_specs=[vmem()] * 2,
        out_specs=vmem(),
        compiler_params=pltpu.CompilerParams(vmem_limit_bytes=4 << 20),
    )(vectors, image)


def halves_kernel(odd, sums1, image1, image2, kept, given):
    sums2 = nt_dot(image2[...], jnp.concatenate([image2[...], image1[...]], axis=0), HIGHEST)
    for when, mine, other in ((0, sums1, None), (1, None, sums1)):

        @pl.when(odd[0] == when)
        def _():
            kept[...] = sums2 if mine is None else mine[...]
            given[...] = sums2 if other is None else other[...]


def halves(odd, sums1, image1, image2):
    shape = jax.ShapeDtypeStruct(sums1.shape, F32)
    return pl.pallas_call(
        halves_kernel,
        out_shape=(shape, shape),
        in_specs=[smem()] + [vmem()] * 3,
        out_specs=(vmem(), vmem()),
        compiler_params=pltpu.CompilerParams(vmem_limit_bytes=4 << 20),
    )(odd, sums1, image1, image2)


def inverse_factors(grams):
    n = grams[0].shape[0]
    wide = 2 * n
    group = 8
    pieces = n // group
    sub = lax.broadcasted_iota(jnp.int32, (group, wide), 0)
    lane = lax.broadcasted_iota(jnp.int32, (group, wide), 1)

    def spread(row):
        return jnp.broadcast_to(row, (group, wide))

    held = []
    for a in grams:
        rows = []
        for r in range(pieces):
            eye = (lane == sub + (n + group * r)).astype(F32)[:, n:]
            rows.append(jnp.concatenate([a[group * r : group * (r + 1), :], eye], axis=1))
        held.append(rows)
    pivots = [[] for _ in grams]
    for k in range(pieces):
        columns = [
            [[spread(m[r][:, j : j + 1]) for r in range(k, pieces)] for j in range(group * k, group * (k + 1))]
            for m in held
        ]
        found = [jnp.ones((group, wide), F32) for _ in grams]
        for j in range(group):
            for p, m in enumerate(held):
                column = columns[p]
                pivot = spread(column[j][0][j : j + 1, :])
                found[p] = jnp.where(sub == j, pivot, found[p])
                scale = 1.0 / pivot
                row = spread(m[k][j : j + 1, :])
                later = [spread(column[i][0][j : j + 1, :]) for i in range(j + 1, group)]
                for r in range(k, pieces):
                    factor = column[j][r - k] * scale
                    if r == k:
                        factor = jnp.where(sub > j, factor, 0.0)
                    m[r] = m[r] - factor * row
                    for i in range(j + 1, group):
                        column[i][r - k] = column[i][r - k] - factor * later[i - j - 1]
        for p in range(len(grams)):
            pivots[p].append(found[p])
    return [
        jnp.concatenate(
            [(held[p][r] / jnp.sqrt(pivots[p][r]))[:, n:] for r in range(pieces)], axis=0
        )
        for p in range(len(grams))
    ]


def diagonal(a):
    n = a.shape[0]
    row = lax.broadcasted_iota(jnp.int32, (n, n), 0)
    lane = lax.broadcasted_iota(jnp.int32, (n, n), 1)
    return jnp.sum(jnp.where(row == lane, a, 0.0), axis=0, keepdims=True)


def in_range(d):
    return (jnp.min(d) > SMALL) & (jnp.max(d) < LARGE)


def factor_kernel(total_rows, odd, kept, received, inverse2, rayleigh, good):
    n = inverse2.shape[0]
    scale = 1.0 / (total_rows**0.5)
    sums1 = jnp.where(odd[0] == 0, kept[...], received[...])
    sums2 = jnp.where(odd[0] == 0, received[...], kept[...])
    gram1, gram2 = [sums[:, :n] * (1.0 / total_rows) for sums in (sums1, sums2)]
    x1, x2 = inverse_factors([gram1, gram2])
    inverse2[...] = x2
    rayleigh[0] = sums1[:, n:].T * scale
    right = nt_dot(sums2[:, n:].T, x1, HIGHEST)
    rayleigh[1] = jnp.dot(x1, right, precision=HIGHEST, preferred_element_type=F32) * scale
    fine = True
    for gram, x in ((gram1, x1), (gram2, x2)):
        d = diagonal(gram)
        fine = fine & in_range(d) & (jnp.sum(x * x * d) < GAIN_LIMIT * n)
    good[0] = fine.astype(jnp.int32)


def factor(total_rows, odd, kept, received):
    n = kept.shape[0]
    return pl.pallas_call(
        functools.partial(factor_kernel, total_rows),
        out_shape=(
            jax.ShapeDtypeStruct((n, n), F32),
            jax.ShapeDtypeStruct((2, n, n), F32),
            pltpu.MemorySpace.SMEM((1,), jnp.int32),
        ),
        in_specs=[smem(), vmem(), vmem()],
        out_specs=(vmem(), vmem(), smem()),
        compiler_params=pltpu.CompilerParams(vmem_limit_bytes=8 << 20),
    )(odd, kept, received)


def from_peer(value, mask):
    devices = lax.axis_size(AXES)
    return lax.ppermute(value, AXES, [(i, i ^ mask) for i in range(devices)])


def sum_halves(kept, given):
    kept = kept + from_peer(given, 1)
    bit, last = 2, lax.axis_size(AXES)
    if last.bit_length() % 2 == 1:
        kept = kept + from_peer(kept, bit)
        bit *= 2
    while bit < last:
        near, far = from_peer(kept, bit), from_peer(kept, 2 * bit)
        kept = (kept + near) + (far + from_peer(kept, 3 * bit))
        bit *= 4
    return kept, from_peer(kept, 1)


def step_by_step(vectors, tiles, counts, tile_col, send_list):
    me = lax.axis_index(AXES)
    outgoing = lax.dynamic_index_in_dim(send_list, me, 0, keepdims=False).reshape(-1)
    devices = lax.axis_size(AXES)
    width, rows_here = vectors.shape
    blocks_here = counts.shape[0]
    tile_size = tiles.shape[1]
    depth = tiles.shape[0] // blocks_here
    total_rows = rows_here * devices
    live = jnp.arange(tiles.shape[0], dtype=jnp.int32) % depth < jnp.repeat(counts, depth)
    live = live.astype(F32)
    current = vectors
    rayleigh = []
    for step in range(ITERS):
        rounded = current.astype(BF16)
        own_blocks = rounded.reshape(width, blocks_here, tile_size).transpose(1, 0, 2)
        parcel = jnp.take(own_blocks, outgoing, axis=0)
        arrived = lax.all_to_all(parcel, AXES, split_axis=0, concat_axis=0, tiled=True)
        picked = jnp.take(arrived, tile_col, axis=0)
        prod = jnp.einsum("jrc,jkc->jkr", tiles, picked, preferred_element_type=F32)
        prod = prod * live[:, None, None]
        image = prod.reshape(blocks_here, depth, width, tile_size).sum(axis=1)
        image = image.transpose(1, 0, 2).reshape(width, rows_here)
        gram_part = jnp.dot(image, image.T, precision=HIGHEST)
        quotient_part = jnp.dot(current, image.T, precision=HIGHEST)
        gram, quotient = lax.psum((gram_part, quotient_part), AXES)
        gram = gram / total_rows
        rayleigh.append(quotient / jnp.sqrt(F32(total_rows)))
        lower = jnp.linalg.cholesky(gram)
        current = lax.linalg.triangular_solve(lower, image, left_side=True, lower=True)
    return current, jnp.stack(rayleigh)


def on_device(vectors, tiles, counts, tile_col, send_list):
    devices = lax.axis_size(AXES)
    total_rows = vectors.shape[1] * devices
    exchange = Exchange(devices, send_list, tiles.shape[1])
    odd = (lax.axis_index(AXES) & 1).reshape(1)
    plan = jnp.concatenate([counts, exchange.arrival(tile_col)])
    arrived, plan, odd = exchange(vectors.astype(BF16), plan, odd)
    image1, rounded = image_of((F32, BF16), plan, arrived, tiles)
    arrived, sums1 = exchange(rounded, first_sums(vectors, image1))
    (image2,) = image_of((F32,), plan, arrived, tiles)
    kept, received = sum_halves(*halves(odd, sums1, image1, image2))
    inverse2, rayleigh, good = factor(total_rows, odd, kept, received)

    def fast():
        return jnp.dot(inverse2, image2, precision=lax.Precision.HIGH), rayleigh

    def slow():
        return step_by_step(vectors, tiles, counts, tile_col, send_list)

    return lax.cond(good[0] > 0, fast, slow)


def solution(mesh):
    return jax.shard_map(
        on_device,
        mesh=mesh,
        in_specs=(
            P(None, AXES),
            P(AXES, None, None),
            P(AXES),
            P(AXES),
            P(),
        ),
        out_specs=(P(None, AXES), P()),
        check_vma=False,
    )
```

```python
import functools

import jax
import jax.numpy as jnp
from jax import lax
from jax.experimental import pallas as pl
from jax.experimental.pallas import tpu as pltpu
from jax.sharding import PartitionSpec as P

ITERS = 2
AXES = ("gx", "gy")
F32 = jnp.float32
BF16 = jnp.bfloat16
HIGHEST = lax.Precision.HIGHEST

GAIN_LIMIT = 1.5
SMALL, LARGE = 1e-25, 1e25
STEP = 4


def vmem():
    return pl.BlockSpec(memory_space=pltpu.VMEM)


def smem():
    return pl.BlockSpec(memory_space=pltpu.SMEM)


def nt_dot(a, b, precision=None):
    return lax.dot_general(
        a, b, (((1,), (1,)), ((), ())), precision=precision, preferred_element_type=F32
    )


def pack_kernel(outgoing, own, other, parcel):
    peers, rows, tile = parcel.shape
    width = own.shape[0]
    slots = rows // width // 2

    def one(p, carry):
        for i, source in enumerate((own, other)):
            for slot in range(slots):
                block = outgoing[(i * peers + p) * slots + slot]
                at = (i * slots + slot) * width
                parcel[p, at : at + width, :] = source[:, pl.ds(pl.multiple_of(block * tile, tile), tile)]
        return carry

    lax.fori_loop(0, peers, one, 0, unroll=8)


def pack(outgoing, own, other, peers, tile):
    width = own.shape[0]
    rows = outgoing.shape[0] // peers * width
    return pl.pallas_call(
        pack_kernel,
        out_shape=jax.ShapeDtypeStruct((peers, rows, tile), BF16),
        in_specs=[smem(), vmem(), vmem()],
        out_specs=vmem(),
        compiler_params=pltpu.CompilerParams(vmem_limit_bytes=4 << 20),
        cost_estimate=pl.CostEstimate(
            flops=5_000_000_000, bytes_accessed=32 << 20, transcendentals=0
        ),
    )(outgoing, own, other)


class Exchange:
    def __init__(self, devices, send_list, tile):
        assert devices >= 4 and devices & (devices - 1) == 0
        self.peers = half = devices // 2
        self.swap = [(i, i ^ half) for i in range(devices)]
        self.groups = [list(range(half)), list(range(half, devices))]
        self.tile = tile
        self.slots = send_list.shape[2]
        me = lax.axis_index(AXES)
        self.side = (me >= half).astype(jnp.int32)
        lists = [
            lax.dynamic_slice(send_list, (source, self.side * half, 0), (1, half, self.slots))
            for source in (me, me ^ half)
        ]
        self.outgoing = jnp.concatenate(lists).reshape(-1)

    def arrival(self, tile_col):
        sender, slot = tile_col // self.slots, tile_col % self.slots
        far = (sender >= self.peers).astype(jnp.int32) ^ self.side
        return (2 * (sender % self.peers) + far) * self.slots + slot

    def __call__(self, rounded, *ahead):
        other = lax.ppermute(rounded, AXES, self.swap)
        parcel = pack(self.outgoing, rounded, other, self.peers, self.tile)
        parcel, *ahead = lax.optimization_barrier((parcel, *ahead))
        arrived = lax.all_to_all(
            parcel, AXES, split_axis=0, concat_axis=0, axis_index_groups=self.groups, tiled=True
        )
        return (arrived.reshape(-1, rounded.shape[0], self.tile), *ahead)


def image_kernel(blocks, plan, arrived, tiles, image, *rounded):
    depth = tiles.shape[0] // blocks
    tile = tiles.shape[1]
    width = arrived.shape[1]
    mxus = (0, 1)

    def push(b, t, register, mxu):
        pltpu.matmul_push_rhs(
            tiles[b * depth + t], staging_register=register, mxu_index=mxu, transpose=True
        )

    def block(b, t):
        found = arrived[plan[blocks + b * depth + t]]
        return jnp.where(t < plan[b], found, jnp.zeros_like(found))

    def run(*refs):
        sums = (refs[0:2], refs[2:4])
        spare = refs[4:6]
        for ref in refs:
            pltpu.matmul_pop(ref)

        def flush(b):
            first, second = sums[b % 2]
            value = pltpu.matmul_pop(first) + pltpu.matmul_pop(second)
            for ref in (image, *rounded):
                ref[:, b * tile : (b + 1) * tile] = value.astype(ref.dtype)

        for mxu in mxus:
            push(0, mxu, 0, mxu)
        for b in range(blocks):
            steps = (plan[b] + STEP - 1) // STEP

            def products(t, push_next):
                for mxu in mxus:
                    push(b, t + 2 + mxu, 1, mxu)
                for mxu in mxus:
                    pltpu.matmul_acc_lhs(sums[b % 2][mxu], block(b, t + mxu), load_staged_rhs=0)
                for mxu in mxus:
                    push_next(mxu)
                for mxu in mxus:
                    pltpu.matmul_acc_lhs(sums[b % 2][mxu], block(b, t + 2 + mxu), load_staged_rhs=1)

            def step(q, carry):
                products(q * STEP, lambda mxu: push(b, (q + 1) * STEP + mxu, 0, mxu))
                return carry

            lax.fori_loop(0, steps - 1, step, 0)
            products((steps - 1) * STEP, lambda mxu: push(min(b + 1, blocks - 1), mxu, 0, mxu))
            if b:
                flush(b - 1)
        for mxu in mxus:
            pltpu.matmul_acc_lhs(spare[mxu], jnp.zeros((16, tile), BF16), load_staged_rhs=0)
        flush(blocks - 1)
        for ref in spare:
            pltpu.matmul_pop(ref)

    pl.run_scoped(
        run,
        *[pltpu.ACC(mxu)((width, tile), F32) for mxu in mxus + mxus],
        *[pltpu.ACC(mxu)((16, tile), F32) for mxu in mxus],
    )


def image_of(kinds, plan, arrived, tiles):
    width, tile = arrived.shape[1:]
    blocks = plan.shape[0] - tiles.shape[0]
    assert tile == 256 and width % 16 == 0 and width <= 256
    assert tiles.shape[0] % (blocks * STEP) == 0
    grant = (4 if 16 * arrived.size <= tiles.size else 24) << 20
    return pl.pallas_call(
        functools.partial(image_kernel, blocks),
        out_shape=[jax.ShapeDtypeStruct((width, blocks * tile), kind) for kind in kinds],
        in_specs=[smem(), vmem(), vmem()],
        out_specs=[vmem()] * len(kinds),
        compiler_params=pltpu.CompilerParams(vmem_limit_bytes=grant),
        cost_estimate=pl.CostEstimate(
            flops=width * tiles.size, bytes_accessed=tiles.size, transcendentals=0
        ),
    )(plan, arrived, tiles)


def first_sums_kernel(vectors, image, sums):
    sums[...] = nt_dot(image[...], jnp.concatenate([image[...], vectors[...]], axis=0), HIGHEST)


def first_sums(vectors, image):
    n = vectors.shape[0]
    return pl.pallas_call(
        first_sums_kernel,
        out_shape=jax.ShapeDtypeStruct((n, 2 * n), F32),
        in_specs=[vmem()] * 2,
        out_specs=vmem(),
        compiler_params=pltpu.CompilerParams(vmem_limit_bytes=4 << 20),
    )(vectors, image)


def halves_kernel(odd, sums1, image1, image2, kept, given):
    sums2 = nt_dot(image2[...], jnp.concatenate([image2[...], image1[...]], axis=0), HIGHEST)
    for when, mine, other in ((0, sums1, None), (1, None, sums1)):

        @pl.when(odd[0] == when)
        def _():
            kept[...] = sums2 if mine is None else mine[...]
            given[...] = sums2 if other is None else other[...]


def halves(odd, sums1, image1, image2):
    shape = jax.ShapeDtypeStruct(sums1.shape, F32)
    return pl.pallas_call(
        halves_kernel,
        out_shape=(shape, shape),
        in_specs=[smem()] + [vmem()] * 3,
        out_specs=(vmem(), vmem()),
        compiler_params=pltpu.CompilerParams(vmem_limit_bytes=4 << 20),
    )(odd, sums1, image1, image2)


def inverse_factors(grams):
    n = grams[0].shape[0]
    wide = 2 * n
    group = 8
    pieces = n // group
    sub = lax.broadcasted_iota(jnp.int32, (group, wide), 0)
    lane = lax.broadcasted_iota(jnp.int32, (group, wide), 1)

    def spread(row):
        return jnp.broadcast_to(row, (group, wide))

    held = []
    for a in grams:
        rows = []
        for r in range(pieces):
            eye = (lane == sub + (n + group * r)).astype(F32)[:, n:]
            rows.append(jnp.concatenate([a[group * r : group * (r + 1), :], eye], axis=1))
        held.append(rows)
    pivots = [[] for _ in grams]
    for k in range(pieces):
        columns = [
            [[spread(m[r][:, j : j + 1]) for r in range(k, pieces)] for j in range(group * k, group * (k + 1))]
            for m in held
        ]
        found = [jnp.ones((group, wide), F32) for _ in grams]
        for j in range(group):
            for p, m in enumerate(held):
                column = columns[p]
                pivot = spread(column[j][0][j : j + 1, :])
                found[p] = jnp.where(sub == j, pivot, found[p])
                scale = 1.0 / pivot
                row = spread(m[k][j : j + 1, :])
                later = [spread(column[i][0][j : j + 1, :]) for i in range(j + 1, group)]
                for r in range(k, pieces):
                    factor = column[j][r - k] * scale
                    if r == k:
                        factor = jnp.where(sub > j, factor, 0.0)
                    m[r] = m[r] - factor * row
                    for i in range(j + 1, group):
                        column[i][r - k] = column[i][r - k] - factor * later[i - j - 1]
        for p in range(len(grams)):
            pivots[p].append(found[p])
    return [
        jnp.concatenate(
            [(held[p][r] / jnp.sqrt(pivots[p][r]))[:, n:] for r in range(pieces)], axis=0
        )
        for p in range(len(grams))
    ]


def diagonal(a):
    n = a.shape[0]
    row = lax.broadcasted_iota(jnp.int32, (n, n), 0)
    lane = lax.broadcasted_iota(jnp.int32, (n, n), 1)
    return jnp.sum(jnp.where(row == lane, a, 0.0), axis=0, keepdims=True)


def in_range(d):
    return (jnp.min(d) > SMALL) & (jnp.max(d) < LARGE)


def factor_kernel(total_rows, odd, kept, received, inverse2, rayleigh, good):
    n = inverse2.shape[0]
    scale = 1.0 / (total_rows**0.5)
    sums1 = jnp.where(odd[0] == 0, kept[...], received[...])
    sums2 = jnp.where(odd[0] == 0, received[...], kept[...])
    gram1, gram2 = [sums[:, :n] * (1.0 / total_rows) for sums in (sums1, sums2)]
    x1, x2 = inverse_factors([gram1, gram2])
    inverse2[...] = x2
    rayleigh[0] = sums1[:, n:].T * scale
    right = nt_dot(sums2[:, n:].T, x1, HIGHEST)
    rayleigh[1] = jnp.dot(x1, right, precision=HIGHEST, preferred_element_type=F32) * scale
    fine = True
    for gram, x in ((gram1, x1), (gram2, x2)):
        d = diagonal(gram)
        fine = fine & in_range(d) & (jnp.sum(x * x * d) < GAIN_LIMIT * n)
    good[0] = fine.astype(jnp.int32)


def factor(total_rows, odd, kept, received):
    n = kept.shape[0]
    return pl.pallas_call(
        functools.partial(factor_kernel, total_rows),
        out_shape=(
            jax.ShapeDtypeStruct((n, n), F32),
            jax.ShapeDtypeStruct((2, n, n), F32),
            pltpu.MemorySpace.SMEM((1,), jnp.int32),
        ),
        in_specs=[smem(), vmem(), vmem()],
        out_specs=(vmem(), vmem(), smem()),
        compiler_params=pltpu.CompilerParams(vmem_limit_bytes=8 << 20),
    )(odd, kept, received)


def from_peer(value, mask):
    devices = lax.axis_size(AXES)
    return lax.ppermute(value, AXES, [(i, i ^ mask) for i in range(devices)])


def sum_halves(kept, given):
    kept = kept + from_peer(given, 1)
    bit = lax.axis_size(AXES)
    while bit > 4:
        bit //= 4
        near, far = from_peer(kept, bit), from_peer(kept, 2 * bit)
        kept = (kept + near) + (far + from_peer(kept, 3 * bit))
    if bit == 4:
        kept = kept + from_peer(kept, 2)
    return kept, from_peer(kept, 1)


def step_by_step(vectors, tiles, counts, tile_col, send_list):
    me = lax.axis_index(AXES)
    outgoing = lax.dynamic_index_in_dim(send_list, me, 0, keepdims=False).reshape(-1)
    devices = lax.axis_size(AXES)
    width, rows_here = vectors.shape
    blocks_here = counts.shape[0]
    tile_size = tiles.shape[1]
    depth = tiles.shape[0] // blocks_here
    total_rows = rows_here * devices
    live = jnp.arange(tiles.shape[0], dtype=jnp.int32) % depth < jnp.repeat(counts, depth)
    live = live.astype(F32)
    current = vectors
    rayleigh = []
    for step in range(ITERS):
        rounded = current.astype(BF16)
        own_blocks = rounded.reshape(width, blocks_here, tile_size).transpose(1, 0, 2)
        parcel = jnp.take(own_blocks, outgoing, axis=0)
        arrived = lax.all_to_all(parcel, AXES, split_axis=0, concat_axis=0, tiled=True)
        picked = jnp.take(arrived, tile_col, axis=0)
        prod = jnp.einsum("jrc,jkc->jkr", tiles, picked, preferred_element_type=F32)
        prod = prod * live[:, None, None]
        image = prod.reshape(blocks_here, depth, width, tile_size).sum(axis=1)
        image = image.transpose(1, 0, 2).reshape(width, rows_here)
        gram_part = jnp.dot(image, image.T, precision=HIGHEST)
        quotient_part = jnp.dot(current, image.T, precision=HIGHEST)
        gram, quotient = lax.psum((gram_part, quotient_part), AXES)
        gram = gram / total_rows
        rayleigh.append(quotient / jnp.sqrt(F32(total_rows)))
        lower = jnp.linalg.cholesky(gram)
        current = lax.linalg.triangular_solve(lower, image, left_side=True, lower=True)
    return current, jnp.stack(rayleigh)


def on_device(vectors, tiles, counts, tile_col, send_list):
    devices = lax.axis_size(AXES)
    total_rows = vectors.shape[1] * devices
    exchange = Exchange(devices, send_list, tiles.shape[1])
    odd = (lax.axis_index(AXES) & 1).reshape(1)
    plan = jnp.concatenate([counts, exchange.arrival(tile_col)])
    arrived, plan, odd = exchange(vectors.astype(BF16), plan, odd)
    image1, rounded = image_of((F32, BF16), plan, arrived, tiles)
    arrived, sums1 = exchange(rounded, first_sums(vectors, image1))
    (image2,) = image_of((F32,), plan, arrived, tiles)
    kept, received = sum_halves(*halves(odd, sums1, image1, image2))
    inverse2, rayleigh, good = factor(total_rows, odd, kept, received)

    def fast():
        return jnp.dot(inverse2, image2, precision=HIGHEST), rayleigh

    def slow():
        return step_by_step(vectors, tiles, counts, tile_col, send_list)

    return lax.cond(good[0] > 0, fast, slow)


def solution(mesh):
    return jax.shard_map(
        on_device,
        mesh=mesh,
        in_specs=(
            P(None, AXES),
            P(AXES, None, None),
            P(AXES),
            P(AXES),
            P(),
        ),
        out_specs=(P(None, AXES), P()),
        check_vma=False,
    )
```
